8 devices in a mesh: model: 8 (over z, y, x, core).
Axes of the slice: x: 2, y: 2, z: 1, core: 2. Of those that a mesh axis runs over, the one named last changes fastest.
Arguments:
- act_in: bfloat16 [2048, 18432], P('model')
- ln_gain: float32 [18432], replicated
- w_q: bfloat16 [18432, 12288], P(None, 'model')
- w_kv: bfloat16 [18432, 512], replicated
- w_o: bfloat16 [12288, 18432], P('model')
- positions: int32 [2048], replicated
Outputs:
- output 1: bfloat16 [2048, 18432], P('model')
- output 2: bfloat16 [2048, 256], replicated
- output 3: bfloat16 [2048, 256], replicated
All inputs are finite; a program needn't handle non-finite values.
Results may differ from the reference program's by a relative error of at most 0.0120546.
Values are sent between devices in bfloat16 or wider.
A program may use at most 1 GiB of HBM per device.

```python
import jax
import jax.numpy as jnp
from jax import lax

TOKENS = 2048
SEQ = 2048
D = 18432
HEADS = 48
HEAD = 256
NORM_EPS = 1e-6


def setup_inputs(seed: int = 0) -> dict:
    rng_keys = jax.random.split(jax.random.key(seed), 6)
    act_in = jax.random.normal(rng_keys[0], (TOKENS, D), jnp.float32).astype(jnp.bfloat16)
    ln_gain = jax.random.uniform(rng_keys[1], (D,), jnp.float32, 0.6, 1.4)
    w_q = (jax.random.normal(rng_keys[2], (D, HEADS * HEAD), jnp.float32) * D ** -0.5).astype(jnp.bfloat16)
    w_kv = (jax.random.normal(rng_keys[3], (D, 2 * HEAD), jnp.float32) * D ** -0.5).astype(jnp.bfloat16)
    out_scale = (SEQ / (HEADS * HEAD)) ** 0.5 / 8.0
    w_o = (jax.random.normal(rng_keys[4], (HEADS * HEAD, D), jnp.float32) * out_scale).astype(jnp.bfloat16)
    positions = jax.random.permutation(rng_keys[5], SEQ).astype(jnp.int32)
    return dict(act_in=act_in, ln_gain=ln_gain, w_q=w_q, w_kv=w_kv, w_o=w_o, positions=positions)


def layer_norm(act_rows, gain_vec):
    rows_f32 = act_rows.astype(jnp.float32)
    row_mean = jnp.mean(rows_f32, axis=-1, keepdims=True)
    centered = rows_f32 - row_mean
    variance = jnp.mean(centered * centered, axis=-1, keepdims=True)
    return (centered * lax.rsqrt(variance + NORM_EPS) * gain_vec).astype(jnp.bfloat16)


def reference(act_in, ln_gain, w_q, w_kv, w_o, positions):
    normed = layer_norm(act_in, ln_gain)
    queries = jnp.dot(normed, w_q, preferred_element_type=jnp.float32).astype(jnp.bfloat16)
    kv_proj = jnp.dot(normed, w_kv, preferred_element_type=jnp.float32).astype(jnp.bfloat16)
    k_cache = kv_proj[:, :HEAD]
    v_cache = kv_proj[:, HEAD:]
    n_seq = TOKENS // SEQ
    visible = positions[None, :] <= positions[:, None]
    q_seqs = queries.reshape(n_seq, SEQ, HEADS, HEAD).transpose(0, 2, 1, 3)
    k_seqs = k_cache.reshape(n_seq, SEQ, HEAD)
    v_seqs = v_cache.reshape(n_seq, SEQ, HEAD)

    def one_seq(operands):
        q_blk, k_blk, v_blk = operands

        def one_head(q_head):
            scores = jnp.dot(q_head, k_blk.T, preferred_element_type=jnp.float32) * HEAD ** -0.5
            scores = jnp.where(visible, scores, -1e30)
            attn_prob = jax.nn.softmax(scores, axis=-1).astype(jnp.bfloat16)
            return jnp.dot(attn_prob, v_blk, preferred_element_type=jnp.float32).astype(jnp.bfloat16)

        return lax.map(one_head, q_blk)

    attended = lax.map(one_seq, (q_seqs, k_seqs, v_seqs))
    attended = attended.transpose(0, 2, 1, 3).reshape(TOKENS, HEADS * HEAD)
    y_out = jnp.dot(attended, w_o, preferred_element_type=jnp.float32).astype(jnp.bfloat16)
    return y_out, k_cache, v_cache
```

```python
import functools

import jax
import jax.numpy as jnp
from jax import lax
from jax.experimental import pallas as pl
from jax.experimental.pallas import tpu as pltpu
from jax.sharding import PartitionSpec as P


NORM_EPS = 1e-6
CORE, XN, YN, DIAG = 1, 2, 4, 6
BF16, F32 = jnp.bfloat16, jnp.float32


def _params(n=1):
    return pltpu.CompilerParams(dimension_semantics=("arbitrary",) * n)


def _norm_kernel(strip, chunk, x_ref, g_ref, *out_refs):
    rows, width = x_ref.shape[-2:]
    n_chunks = width // chunk

    def chunk_of(ref, r, c):
        return ref[0, pl.ds(pl.multiple_of(r * strip, strip), strip), pl.ds(pl.multiple_of(c * chunk, chunk), chunk)]

    def fold(v):
        acc = v[:, :128]
        for i in range(1, chunk // 128):
            acc = acc + v[:, i * 128:(i + 1) * 128]
        return acc

    def one_piece(out_ref):
        def one_strip(r, _):
            def add_sum(c, acc):
                return acc + fold(chunk_of(x_ref, r, c).astype(F32))

            total = lax.fori_loop(0, n_chunks, add_sum, jnp.zeros((strip, 128), F32))
            mean = jnp.sum(total, axis=1, keepdims=True) / width

            def add_sq(c, acc):
                d = chunk_of(x_ref, r, c).astype(F32) - mean
                return acc + fold(d * d)

            sq = lax.fori_loop(0, n_chunks, add_sq, jnp.zeros((strip, 128), F32))
            rstd = lax.rsqrt(jnp.sum(sq, axis=1, keepdims=True) / width + NORM_EPS)

            def put(c, _):
                d = chunk_of(x_ref, r, c).astype(F32) - mean
                cols = pl.ds(pl.multiple_of(c * chunk, chunk), chunk)
                out_ref[pl.ds(pl.multiple_of(r * strip, strip), strip), cols] = (d * rstd * g_ref[:, cols]).astype(BF16)
                return 0

            lax.fori_loop(0, n_chunks, put, 0)
            return 0

        lax.fori_loop(0, rows // strip, one_strip, 0)

    for i, out_ref in enumerate(out_refs):
        pl.when(pl.program_id(0) == i)(functools.partial(one_piece, out_ref))


def norm_pieces(x4, gain, first, step, count):
    _, rows, width = x4.shape
    return pl.pallas_call(
        functools.partial(_norm_kernel, 16, 1024),
        grid=(count,),
        in_specs=[
            pl.BlockSpec((1, rows, width), lambda i: (first + step * i, 0, 0)),
            pl.BlockSpec((1, width), lambda i: (0, 0)),
        ],
        out_specs=[pl.BlockSpec((rows, width), lambda i: (0, 0))] * count,
        out_shape=[jax.ShapeDtypeStruct((rows, width), BF16)] * count,
        compiler_params=_params(),
        cost_estimate=pl.CostEstimate(flops=8 * count * rows * width, bytes_accessed=4 * count * rows * width, transcendentals=0),
        name="norm",
    )(x4, gain)


def _stack_dot_kernel(n_lhs, *refs):
    lhs, (w_ref, out_ref, acc_ref) = refs[:n_lhs], refs[n_lhs:]
    step = pl.program_id(0)
    stacked = jnp.concatenate([r[...] for r in lhs], axis=0)
    part = jnp.dot(stacked, w_ref[...], preferred_element_type=F32)

    @pl.when(step == 0)
    def _():
        acc_ref[...] = part

    @pl.when(step > 0)
    def _():
        acc_ref[...] += part

    @pl.when(step == pl.num_programs(0) - 1)
    def _():
        out_ref[...] = acc_ref[...].astype(BF16)


def stack_dot(lhs, w, depth):
    rows, width = lhs[0].shape
    total, cols = rows * len(lhs), w.shape[1]
    return pl.pallas_call(
        functools.partial(_stack_dot_kernel, len(lhs)),
        grid=(width // depth,),
        in_specs=[pl.BlockSpec((rows, depth), lambda k: (0, k))] * len(lhs) + [pl.BlockSpec((depth, cols), lambda k: (k, 0))],
        out_specs=pl.BlockSpec((total, cols), lambda k: (0, 0)),
        out_shape=jax.ShapeDtypeStruct((total, cols), BF16),
        scratch_shapes=[pltpu.VMEM((total, cols), F32)],
        compiler_params=_params(),
        cost_estimate=pl.CostEstimate(flops=2 * total * width * cols, bytes_accessed=2 * (total * width + width * cols), transcendentals=0),
    )(*lhs, w)


def _unit_kernel(n_lhs, kc, nc, qs, os_, *refs):
    h_refs, (wq, wo, k_hbm, v_hbm, qpos, kpos), refs = refs[:n_lhs], refs[n_lhs:n_lhs + 6], refs[n_lhs + 6:]
    outs, (wq_buf, h_buf, acc, q_buf, o_buf, wo_buf, y_buf, k_buf, v_buf, wq_sem, h_sem, wo_sem, y_sem, kv_sem) = refs[:-14], refs[-14:]
    piece, width = h_refs[0].shape
    _, proj = acc.shape
    head = k_buf.shape[1]
    n_q, n_o = width // kc, wo.shape[1] // nc

    def q_copies(i, slot):
        cols = pl.ds(pl.multiple_of(i * kc, kc), kc)
        cps = [pltpu.make_async_copy(wq.at[cols, :], wq_buf.at[slot], wq_sem.at[slot])]
        for j, h in enumerate(h_refs):
            cps.append(pltpu.make_async_copy(h.at[:, cols], h_buf.at[slot, pl.ds(j * piece, piece), :], h_sem.at[slot, j]))
        return cps

    def o_copy(i, slot):
        return pltpu.make_async_copy(wo.at[:, pl.ds(pl.multiple_of(i * nc, nc), nc)], wo_buf.at[slot], wo_sem.at[slot])

    def y_copies(i, slot):
        cols = pl.ds(pl.multiple_of(i * nc, nc), nc)
        cps, at = [], 0
        for j, out in enumerate(outs):
            n = out.shape[0]
            cps.append(pltpu.make_async_copy(y_buf.at[slot, pl.ds(at, n), :], out.at[:, cols], y_sem.at[slot, j]))
            at += n
        return cps

    for i in range(qs):
        for c in q_copies(i, i):
            c.start()
    kv = [pltpu.make_async_copy(k_hbm, k_buf, kv_sem.at[0]), pltpu.make_async_copy(v_hbm, v_buf, kv_sem.at[1])]
    for c in kv:
        c.start()
    acc[...] = jnp.zeros_like(acc)

    def q_step(i, _):
        slot = lax.rem(i, qs)
        for c in q_copies(i, slot):
            c.wait()
        acc[...] += jnp.dot(h_buf[slot], wq_buf[slot], preferred_element_type=F32)

        @pl.when(i + qs < n_q)
        def _():
            for c in q_copies(i + qs, slot):
                c.start()

        return 0

    lax.fori_loop(0, n_q, q_step, 0)
    for i in range(os_):
        o_copy(i, i).start()
    q_buf[...] = acc[...].astype(BF16)
    for c in kv:
        c.wait()

    def one_head(n, _):
        cols = pl.ds(pl.multiple_of(n * head, head), head)
        s = lax.dot_general(q_buf[:, cols], k_buf[...], (((1,), (1,)), ((), ())), preferred_element_type=F32)
        s = jnp.where(kpos[...] <= qpos[...], s, -1e30)
        top = jnp.max(s, axis=-1, keepdims=True)
        e = jnp.exp((s - top) * (head ** -0.5))
        p = (e * (1.0 / jnp.sum(e, axis=-1, keepdims=True))).astype(BF16)
        o_buf[:, cols] = jnp.dot(p, v_buf[...], preferred_element_type=F32).astype(BF16)
        return 0

    lax.fori_loop(0, proj // head, one_head, 0)


    def o_step(i, _):
        slot, yslot = lax.rem(i, os_), lax.rem(i, 2)
        o_copy(i, slot).wait()

        @pl.when(i >= 2)
        def _():
            for c in y_copies(i - 2, yslot):
                c.wait()

        y_buf[yslot] = jnp.dot(o_buf[...], wo_buf[slot], preferred_element_type=F32).astype(BF16)
        for c in y_copies(i, yslot):
            c.start()

        @pl.when(i + os_ < n_o)
        def _():
            o_copy(i + os_, slot).start()

        return 0

    lax.fori_loop(0, n_o, o_step, 0)
    for i in (n_o - 2, n_o - 1):
        for c in y_copies(i, i % 2):
            c.wait()


def unit_call(hs, wq, wo, k, v, qpos, kpos, index, splits, kc=1024, nc=1024, qs=4, os_=3):
    piece, width = hs[0].shape
    n = len(hs)
    rows = piece * n
    proj = wq.shape[1]
    keys, head = k.shape
    any_ = pl.BlockSpec(memory_space=pl.ANY)
    heads = proj // head
    return pl.pallas_call(
        functools.partial(_unit_kernel, n, kc, nc, qs, os_),
        grid=(1,),
        in_specs=[any_] * (n + 4) + [pl.BlockSpec((rows, 1), lambda i: (index, 0)), pl.BlockSpec((1, keys), lambda i: (0, 0))],
        out_specs=[any_] * len(splits),
        out_shape=[jax.ShapeDtypeStruct((r, width), BF16) for r in splits],
        scratch_shapes=[
            pltpu.VMEM((qs, kc, proj), BF16), pltpu.VMEM((qs, rows, kc), BF16), pltpu.VMEM((rows, proj), F32),
            pltpu.VMEM((rows, proj), BF16), pltpu.VMEM((rows, proj), BF16), pltpu.VMEM((os_, proj, nc), BF16),
            pltpu.VMEM((2, rows, nc), BF16), pltpu.VMEM((keys, head), BF16), pltpu.VMEM((keys, head), BF16),
            pltpu.SemaphoreType.DMA((qs,)), pltpu.SemaphoreType.DMA((qs, n)), pltpu.SemaphoreType.DMA((os_,)),
            pltpu.SemaphoreType.DMA((2, len(splits))), pltpu.SemaphoreType.DMA((2,)),
        ],
        compiler_params=pltpu.CompilerParams(dimension_semantics=("arbitrary",)),
        cost_estimate=pl.CostEstimate(flops=2 * rows * proj * (2 * width + 2 * keys), bytes_accessed=2 * (2 * width * proj + 2 * rows * width), transcendentals=rows * keys * heads),
        name="unit",
    )(*hs, wq, wo, k, v, qpos, kpos)


def add(*terms):
    total = terms[0].astype(F32)
    for t in terms[1:]:
        total = total + t.astype(F32)
    return total.astype(BF16)


UNITS = ("u1a", "u1b", "u2a", "u2b", "u3a", "u3b", "u0a", "u0b")


def solution(mesh):
    n_dev = mesh.shape["model"]

    def send(value, mask):
        return lax.ppermute(value, "model", [(i, i ^ mask) for i in range(n_dev)])

    def by_mask(arr, me):
        cube = arr.reshape((2, 2, 2) + arr.shape[1:])
        for axis, bit in ((0, 4), (1, 2), (2, 1)):
            cube = jnp.where((me & bit) != 0, jnp.flip(cube, axis), cube)
        return cube.reshape(arr.shape)

    def local_step(x_loc, ln_gain, wq_loc, w_kv, wo_loc, positions):
        me = lax.axis_index("model")
        rows, width = x_loc.shape
        head = w_kv.shape[1] // 2
        seq = positions.shape[0]
        piece = rows // 4
        x4 = x_loc.reshape(4, piece, width)
        gain = ln_gain.reshape(1, width)

        h, fx, fy, fd = [None] * 4, [None] * 4, [None] * 4, [None] * 4
        h[0], h[2] = norm_pieces(x4, gain, 0, 2, 2)
        fx[0], fy[2] = send(h[0], XN), send(h[2], YN)
        h[1], h[3] = norm_pieces(x4, gain, 1, 2, 2)
        kv = stack_dot(h, w_kv, 2048)
        kv_m = [kv] + [None] * 7
        for m in (XN, YN, DIAG):
            kv_m[m] = send(kv, m)
        fx[1], fy[3] = send(h[1], XN), send(h[3], YN)
        fx[2], fy[0] = send(h[2], XN), send(h[0], YN)
        fx[3], fy[1] = send(h[3], XN), send(h[1], YN)
        fd[0], fd[2] = send(fx[0], YN), send(fy[2], XN)
        fd[1], fd[3] = send(fx[1], YN), send(fy[3], XN)
        for m in (0, XN, YN, DIAG):
            kv_m[m | CORE] = send(kv_m[m], CORE)

        kv_all = by_mask(jnp.stack(kv_m), me).reshape(seq, 2 * head)
        k_cache, v_cache = kv_all[:, :head], kv_all[:, head:]
        pos_m = by_mask(positions.reshape(n_dev, 4, piece), me)
        kpos = positions.reshape(1, seq)
        plan = {
            "u0a": ((0, 0, h[0]), (0, 2, h[2])), "u0b": ((0, 1, h[1]), (0, 3, h[3])),
            "u1a": ((XN, 0, fx[0]), (YN, 2, fy[2])), "u1b": ((XN, 1, fx[1]), (YN, 3, fy[3])),
            "u2a": ((XN, 2, fx[2]), (YN, 0, fy[0])), "u2b": ((XN, 3, fx[3]), (YN, 1, fy[1])),
            "u3a": ((DIAG, 0, fd[0]), (DIAG, 2, fd[2])), "u3b": ((DIAG, 1, fd[1]), (DIAG, 3, fd[3])),
        }
        qpos = jnp.concatenate([pos_m[m | c, i] for u in UNITS for c in (0, CORE) for m, i, _ in plan[u]]).reshape(-1, 1)

        def unit(name):
            mine = [b[2] for b in plan[name]]
            swapped = [send(b, CORE) for b in mine]
            ya, yb, other = unit_call(mine + swapped, wq_loc, wo_loc, k_cache, v_cache, qpos, kpos, UNITS.index(name), [piece, piece, 2 * piece])
            back = send(other, CORE)
            return (ya, back[:piece]), (yb, back[piece:])

        x0, y2 = unit("u1a")
        x1, y3 = unit("u1b")
        x2, y0 = unit("u2a")
        x3, y1 = unit("u2b")
        d0, d2 = unit("u3a")
        d1, d3 = unit("u3b")
        o0, o2 = unit("u0a")
        o1, o3 = unit("u0b")

        rx0, ry2 = send(add(*x0), XN), send(add(*y2), YN)
        rx1, ry3 = send(add(*x1), XN), send(add(*y3), YN)
        hx0, hy2 = send(add(*d0), XN), send(add(*d2), YN)
        hx1, hy3 = send(add(*d1), XN), send(add(*d3), YN)
        ry0, rx2 = send(add(*y0, hx0), YN), send(add(*x2, hy2), XN)
        ry1, rx3 = send(add(*y1, hx1), YN), send(add(*x3, hy3), XN)
        y_loc = jnp.concatenate([add(*o0, rx0, ry0), add(*o1, rx1, ry1), add(*o2, rx2, ry2), add(*o3, rx3, ry3)], axis=0)
        return y_loc, k_cache, v_cache

    return jax.shard_map(
        local_step,
        mesh=mesh,
        in_specs=(P("model", None), P(None), P(None, "model"), P(None, None), P("model", None), P(None)),
        out_specs=(P("model", None), P(None, None), P(None, None)),
        check_vma=False,
    )
```

```python
import functools
import math

import jax
import jax.numpy as jnp
from jax import lax
from jax.experimental import pallas as pl
from jax.experimental.pallas import tpu as pltpu
from jax.sharding import PartitionSpec as P


NORM_EPS = 1e-6
LOG2E = math.log2(math.e)
VMEM_BYTES = 67043328
NORM_BYTES = 56 << 20
AXIS = "model"
CORE, XN, YN, DIAG = 1, 2, 4, 6
BF16, F32 = jnp.bfloat16, jnp.float32


def _norm_kernel(chunk, steps, x_ref, g_ref, *out_refs):
    rows, width = x_ref.shape
    n_chunks = width // chunk

    def cols(c):
        return pl.ds(pl.multiple_of(c * chunk, chunk), chunk)

    def load(c):
        return x_ref[:, cols(c)].astype(F32)

    def fold(v):
        acc = v[:, :128]
        for i in range(1, chunk // 128):
            acc = acc + v[:, i * 128:(i + 1) * 128]
        return acc

    def square(c, acc):
        d = load(c) - mean
        return acc + fold(d * d)

    zero = jnp.zeros((rows, 128), F32)
    mean = jnp.sum(lax.fori_loop(0, n_chunks, lambda c, acc: acc + fold(load(c)), zero), axis=1, keepdims=True) / width
    rstd = lax.rsqrt(jnp.sum(lax.fori_loop(0, n_chunks, square, zero), axis=1, keepdims=True) / width + NORM_EPS)
    for i, out_ref in enumerate(out_refs):
        @pl.when(pl.program_id(0) // steps == i)
        def _():
            def put(c, _):
                out_ref[:, cols(c)] = ((load(c) - mean) * rstd * g_ref[:, cols(c)]).astype(BF16)
                return 0

            lax.fori_loop(0, n_chunks, put, 0)


def _norm_first_kernel(chunk, x_hbm, g_hbm, out_ref, x_buf, g_buf, sem):
    copies = [pltpu.make_async_copy(x_hbm.at[pl.ds(0, x_buf.shape[0]), :], x_buf, sem.at[0]), pltpu.make_async_copy(g_hbm, g_buf, sem.at[1])]
    for c in copies:
        c.start()
    for c in copies:
        c.wait()
    _norm_kernel(chunk, 1, x_buf, g_buf, out_ref)


def norm_first(x, gain, rows):
    width = x.shape[1]
    hbm = pl.BlockSpec(memory_space=pltpu.HBM)
    return pl.pallas_call(
        functools.partial(_norm_first_kernel, 2048),
        grid=(1,),
        in_specs=[hbm, hbm],
        out_specs=pl.BlockSpec(memory_space=pltpu.VMEM),
        out_shape=pltpu.VMEM((rows, width), BF16),
        scratch_shapes=[pltpu.VMEM((rows, width), BF16), pltpu.VMEM(gain.shape, F32), pltpu.SemaphoreType.DMA((2,))],
        compiler_params=pltpu.CompilerParams(dimension_semantics=("arbitrary",), vmem_limit_bytes=NORM_BYTES),
        cost_estimate=pl.CostEstimate(flops=8 * rows * width, bytes_accessed=4 * rows * width, transcendentals=0),
        name="norm",
    )(x, gain)


def norm_rows(x, gain, first, piece, count, rows, stride=1):
    width = x.shape[1]
    steps = piece // rows

    def out_map(i):
        return lambda s: (jnp.clip(s - i * steps, 0, steps - 1), 0)

    return pl.pallas_call(
        functools.partial(_norm_kernel, 2048, steps),
        grid=(count * steps,),
        in_specs=[pl.BlockSpec((rows, width), lambda s: (first // rows + stride * s, 0)), pl.BlockSpec((1, width), lambda s: (0, 0))],
        out_specs=[pl.BlockSpec((rows, width), out_map(i)) for i in range(count)],
        out_shape=[jax.ShapeDtypeStruct((piece, width), BF16)] * count,
        compiler_params=pltpu.CompilerParams(dimension_semantics=("arbitrary",), vmem_limit_bytes=NORM_BYTES),
        cost_estimate=pl.CostEstimate(flops=8 * count * piece * width, bytes_accessed=4 * count * piece * width, transcendentals=0),
        name="norm",
    )(x, gain)


def _order_kernel(n, *refs):
    me = lax.axis_index(AXIS)
    for i in range(2):
        blocks, out = refs[i * n:(i + 1) * n], refs[2 * n + i]
        rows = blocks[0].shape[0]
        for m, block in enumerate(blocks):
            out[pl.ds(pl.multiple_of((me ^ m) * rows, rows), rows), :] = block[...]


def order_blocks(k_blocks, v_blocks):
    n = len(k_blocks)
    rows, cols = k_blocks[0].shape
    return pl.pallas_call(
        functools.partial(_order_kernel, n),
        in_specs=[pl.BlockSpec(memory_space=pltpu.VMEM)] * (2 * n),
        out_specs=[pl.BlockSpec(memory_space=pltpu.VMEM)] * 2,
        out_shape=[jax.ShapeDtypeStruct((rows * n, cols), BF16)] * 2,
        cost_estimate=pl.CostEstimate(flops=2 * rows * n * cols, bytes_accessed=8 * rows * n * cols, transcendentals=0),
        name="order",
    )(*k_blocks, *v_blocks)


def _unit_kernel(names, parts, n_lhs, n_out, index, *flat):
    r = dict(zip(names, flat))
    lhs = [r[f"lhs{i}"] for i in range(n_lhs)]
    outs = [r[f"out{i}"] for i in range(n_out)]
    ring, ring_sem, q_buf = r["ring"], r["ring_sem"], r["q_buf"]
    slots, chunk = ring.shape[:2]
    do_q, do_o = "q" in parts, "o" in parts
    rows, proj = q_buf.shape
    n_q = r["wq"].shape[0] // chunk if do_q else 0
    n_o = r["wo"].shape[1] // chunk if do_o else 0
    total = n_q + n_o

    def at(i):
        return pl.ds(pl.multiple_of(i * chunk, chunk), chunk)

    def wq_copy(i, slot):
        return pltpu.make_async_copy(r["wq"].at[at(i), :], ring.at[slot], ring_sem.at[slot])

    def wo_copy(i, slot):
        return pltpu.make_async_copy(r["wo"].at[:, at(i - n_q)], ring.at[slot], ring_sem.at[slot])

    def h_copies(i, slot):
        cps, first = [], 0
        for j, h in enumerate(lhs):
            n = h.shape[0]
            cps.append(pltpu.make_async_copy(h.at[:, at(i)], r["h_buf"].at[slot, pl.ds(first, n), :], r["h_sem"].at[slot, j]))
            first += n
        return cps

    def y_copies(i, slot):
        cps, first = [], 0
        for j, out in enumerate(outs):
            n = out.shape[0]
            cps.append(pltpu.make_async_copy(r["y_buf"].at[slot, pl.ds(first, n), :], out.at[:, at(i)], r["y_sem"].at[slot, j]))
            first += n
        return cps

    def fetch(i, slot):
        if do_q:
            @pl.when(i < n_q)
            def _():
                wq_copy(i, slot).start()
                for c in h_copies(i, slot):
                    c.start()
        if do_o:
            @pl.when((i >= n_q) & (i < total))
            def _():
                wo_copy(i, slot).start()

    for i in range(slots):
        if i < n_q:
            wq_copy(i, i).start()
            for c in h_copies(i, i):
                c.start()
        elif i < total:
            wo_copy(i, i).start()
    extra = []
    if do_o:
        row, col = (lax.broadcasted_iota(jnp.int32, (rows, rows), d) for d in (0, 1))
        mine = jnp.where(row == col, r["qpos"][index:index + 1, :], 0.0)
        r["q_col"][...] = jnp.sum(mine, axis=1, keepdims=True)
        for i, (name, buf) in enumerate((("k", r["k_buf"]), ("v", r["v_buf"]))):
            n = r["kv_sem"].shape[1]
            for m in range(n):
                block = r[f"{name}{m}"]
                rows_m = block.shape[0]
                extra.append(pltpu.make_async_copy(block, buf.at[pl.ds(m * rows_m, rows_m), :], r["kv_sem"].at[i, m]))
    for c in extra:
        c.start()

    if do_q:
        acc = r["acc"]
        acc[...] = jnp.zeros_like(acc)

        def q_step(i, _):
            slot = lax.rem(i, slots)
            wq_copy(i, slot).wait()
            for c in h_copies(i, slot):
                c.wait()
            acc[...] += jnp.dot(r["h_buf"][slot], ring[slot], preferred_element_type=F32)
            fetch(i + slots, slot)
            return 0

        lax.fori_loop(0, n_q, q_step, 0)
        if not do_o:
            cols = proj // n_out
            for i, out in enumerate(outs):
                out[...] = acc[:, i * cols:(i + 1) * cols].astype(BF16)
            return
        q_buf[...] = acc[...].astype(BF16)

    for c in extra:
        c.wait()
    k_buf, v_buf, o_buf, y_buf = r["k_buf"], r["v_buf"], r["o_buf"], r["y_buf"]
    head = k_buf.shape[1]
    heads = proj // head

    half = rows // 2

    def score(s_ref, n, b):
        cols = pl.ds(pl.multiple_of(n * head, head), head)
        s_ref[...] = lax.dot_general(q_buf[pl.ds(b * half, half), cols], k_buf[...], (((1,), (1,)), ((), ())), preferred_element_type=F32)

    def attend(s_ref, n, b):
        mine, cols = pl.ds(b * half, half), pl.ds(pl.multiple_of(n * head, head), head)
        s = jnp.where(r["kpos"][...] <= r["q_col"][mine, :], s_ref[...], -1e30)
        e = jnp.exp2((s - jnp.max(s, axis=-1, keepdims=True)) * (head ** -0.5 * LOG2E))
        p = (e * (1.0 / jnp.sum(e, axis=-1, keepdims=True))).astype(BF16)
        o_buf[mine, cols] = jnp.dot(p, v_buf[...], preferred_element_type=F32).astype(BF16)

    def one_head(n, _):
        score(r["s_b"], n, 1)
        attend(r["s_a"], n, 0)
        score(r["s_a"], jnp.minimum(n + 1, heads - 1), 0)
        attend(r["s_b"], n, 1)
        return 0

    score(r["s_a"], 0, 0)
    lax.fori_loop(0, heads, one_head, 0)

    def o_step(i, _):
        slot, yslot = lax.rem(n_q + i, slots), lax.rem(i, 2)
        wo_copy(n_q + i, slot).wait()

        @pl.when(i >= 2)
        def _():
            for c in y_copies(i - 2, yslot):
                c.wait()

        y_buf[yslot] = jnp.dot(o_buf[...], ring[slot], preferred_element_type=F32).astype(BF16)
        for c in y_copies(i, yslot):
            c.start()
        fetch(n_q + i + slots, slot)
        return 0

    lax.fori_loop(0, n_o, o_step, 0)
    for i in (n_o - 2, n_o - 1):
        for c in y_copies(i, i % 2):
            c.wait()


def unit_call(lhs, wq, wo, keys, values, qpos, kpos, index, splits, slots=7, chunk=None):
    parts = ("q" if wq is not None else "") + ("o" if wo is not None else "")
    rows = sum(h.shape[0] for h in lhs)
    proj = wq.shape[1]
    width = wq.shape[0]
    chunk = chunk or proj
    any_ = pl.BlockSpec(memory_space=pl.ANY)
    ins = [(f"lhs{i}", h, any_) for i, h in enumerate(lhs)]
    scratch = [("ring", pltpu.VMEM((slots, chunk, proj), BF16)), ("ring_sem", pltpu.SemaphoreType.DMA((slots,))), ("q_buf", pltpu.VMEM((rows, proj), BF16))]
    flops, moved = 0, 0
    if wq is not None:
        ins.append(("wq", wq, any_))
        scratch += [("h_buf", pltpu.VMEM((slots, rows, chunk), BF16)), ("h_sem", pltpu.SemaphoreType.DMA((slots, len(lhs)))), ("acc", pltpu.VMEM((rows, proj), F32))]
        flops += 2 * rows * proj * width
        moved += 2 * (rows + proj) * width
    if wo is not None:
        n_keys, head = kpos.shape[1], keys[0].shape[1]
        ins.append(("wo", wo, any_))
        ins += [(f"k{m}", k, any_) for m, k in enumerate(keys)] + [(f"v{m}", v, any_) for m, v in enumerate(values)]
        ins += [("qpos", qpos, pl.BlockSpec(qpos.shape, lambda i: (0, 0))), ("kpos", kpos, pl.BlockSpec((1, n_keys), lambda i: (0, 0)))]
        scratch += [
            ("o_buf", pltpu.VMEM((rows, proj), BF16)), ("y_buf", pltpu.VMEM((2, rows, chunk), BF16)), ("y_sem", pltpu.SemaphoreType.DMA((2, len(splits)))),
            ("q_col", pltpu.VMEM((rows, 1), F32)), ("s_a", pltpu.VMEM((rows // 2, n_keys), F32)), ("s_b", pltpu.VMEM((rows // 2, n_keys), F32)),
            ("k_buf", pltpu.VMEM((n_keys, head), BF16)), ("v_buf", pltpu.VMEM((n_keys, head), BF16)), ("kv_sem", pltpu.SemaphoreType.DMA((2, len(keys)))),
        ]
        flops += 2 * rows * proj * (width + 2 * n_keys)
        moved += 2 * (rows + proj) * width
        outs = [((n, width), any_) for n in splits]
    else:
        outs = [((rows, n), pl.BlockSpec((rows, n), lambda i: (0, 0))) for n in splits]
    names = [i[0] for i in ins] + [f"out{i}" for i in range(len(outs))] + [s[0] for s in scratch]
    res = pl.pallas_call(
        functools.partial(_unit_kernel, names, parts, len(lhs), len(outs), index),
        grid=(1,),
        in_specs=[i[2] for i in ins],
        out_specs=[o[1] for o in outs],
        out_shape=[jax.ShapeDtypeStruct(o[0], BF16) for o in outs],
        scratch_shapes=[s[1] for s in scratch],
        compiler_params=pltpu.CompilerParams(dimension_semantics=("arbitrary",), vmem_limit_bytes=VMEM_BYTES if wo is not None else NORM_BYTES),
        cost_estimate=pl.CostEstimate(flops=flops, bytes_accessed=moved, transcendentals=0),
    )(*[i[1] for i in ins])
    return res


def _sums_kernel(jobs, n_in, *refs):
    ins, outs, bufs, in_sem, out_sem = refs[:n_in], refs[n_in:-3], refs[-3], refs[-2], refs[-1]
    halves = in_sem.shape[0]
    width = bufs.shape[1] // halves
    loads, stores, slots = {}, [], []
    at = 0
    for out, first, rows, terms in jobs:
        slots.append([])
        for _ in terms:
            slots[-1].append(at)
            at += rows
    n = 0
    for c in range(halves):
        cols = pl.ds(c * width, width)
        n = 0
        for j, (_, _, rows, terms) in enumerate(jobs):
            for i, (ref, first) in enumerate(terms):
                loads[c, j, i] = pltpu.make_async_copy(ins[ref].at[pl.ds(first, rows), cols], bufs.at[pl.ds(slots[j][i], rows), cols], in_sem.at[c, n])
                loads[c, j, i].start()
                n += 1
    for c in range(halves):
        for j, (out, first, rows, terms) in enumerate(jobs):
            for i in range(len(terms)):
                loads[c, j, i].wait()

            def some(k, _):
                cols = pl.ds(pl.multiple_of(c * width + k * 512, 512), 512)
                total = bufs[pl.ds(slots[j][0], rows), cols].astype(F32)
                for at in slots[j][1:]:
                    total = total + bufs[pl.ds(at, rows), cols].astype(F32)
                bufs[pl.ds(slots[j][0], rows), cols] = total.astype(BF16)
                return 0

            lax.fori_loop(0, width // 512, some, 0)
            cols = pl.ds(c * width, width)
            stores.append(pltpu.make_async_copy(bufs.at[pl.ds(slots[j][0], rows), cols], outs[out].at[pl.ds(first, rows), cols], out_sem.at[c, j]))
            stores[-1].start()
    for c in stores:
        c.wait()


def sums(jobs, out_rows, into=None):
    arrays = [] if into is None else [into]
    spec = []
    for out, first, rows, terms in jobs:
        at = []
        for a, f in terms:
            k = next((k for k, b in enumerate(arrays) if b is a), len(arrays))
            if k == len(arrays):
                arrays.append(a)
            at.append((k, f))
        spec.append((out, first, rows, tuple(at)))
    width = arrays[0].shape[1]
    n_terms = sum(len(j[3]) for j in jobs)
    rows_in = sum(j[2] * len(j[3]) for j in jobs)
    any_ = pl.BlockSpec(memory_space=pl.ANY)
    return pl.pallas_call(
        functools.partial(_sums_kernel, tuple(spec), len(arrays)),
        in_specs=[any_] * len(arrays),
        out_specs=[any_] * len(out_rows),
        out_shape=[jax.ShapeDtypeStruct((r, width), BF16) for r in out_rows],
        input_output_aliases={} if into is None else {0: 0},
        scratch_shapes=[pltpu.VMEM((rows_in, width), BF16), pltpu.SemaphoreType.DMA((2, n_terms)), pltpu.SemaphoreType.DMA((2, len(jobs)))],
        compiler_params=pltpu.CompilerParams(vmem_limit_bytes=VMEM_BYTES),
        cost_estimate=pl.CostEstimate(flops=rows_in * width, bytes_accessed=4 * rows_in * width, transcendentals=0),
        name="sums",
    )(*arrays)


def _where_kernel(q_ref, k_ref, q_out, k_out):
    q_out[...] = q_ref[...].astype(F32)
    k_out[...] = k_ref[...].astype(F32)


def as_float(q, k):
    return pl.pallas_call(
        _where_kernel,
        in_specs=[pl.BlockSpec(memory_space=pltpu.VMEM)] * 2,
        out_specs=[pl.BlockSpec(memory_space=pltpu.VMEM)] * 2,
        out_shape=[jax.ShapeDtypeStruct(q.shape, F32), jax.ShapeDtypeStruct(k.shape, F32)],
        cost_estimate=pl.CostEstimate(flops=q.size, bytes_accessed=16 * q.size, transcendentals=0),
        name="where",
    )(q, k)


CUTS = (16, 32, 16)
UNITS = U1A, U1B, U2A, U2B, U3A, U3B, U0A, U0B = ("u1a", "u1b", "u2a", "u2b", "u3a", "u3b", "u0a", "u0b")


def solution(mesh):
    n_dev = mesh.shape[AXIS]

    def send(value, mask):
        return lax.ppermute(value, AXIS, [(i, i ^ mask) for i in range(n_dev)])

    def by_mask(arr, me):
        cube = arr.reshape((2, 2, 2) + arr.shape[1:])
        for axis, bit in ((0, 4), (1, 2), (2, 1)):
            cube = jnp.where((me & bit) != 0, jnp.flip(cube, axis), cube)
        return cube.reshape(arr.shape)

    def local_step(x_loc, ln_gain, wq_loc, w_kv, wo_loc, positions):
        me = lax.axis_index(AXIS)
        rows, width = x_loc.shape
        seq, head = positions.shape[0], w_kv.shape[1] // 2
        piece = rows // 4
        gain = ln_gain.reshape(1, width)

        def send_all(values, mask):
            return [send(v, mask) for v in values]

        h, fx, fy, fd = [[] for _ in range(4)], [None] * 4, [None] * 4, [None] * 4
        a, b, _ = CUTS
        early = norm_first(x_loc, gain, a)
        middle, = norm_rows(x_loc, gain, a, b, 1, a)
        head_rows, tail_rows = norm_rows(x_loc, gain, 0, a, 2, a, (a + b) // a)
        h[0] = [head_rows, middle, tail_rows]
        for i, v in enumerate(norm_rows(x_loc, gain, piece, piece, 3, piece // 2)):
            h[i + 1].append(v)
        k_own, v_own = unit_call(sum(h, []), w_kv, None, None, None, None, None, 0, [head, head], slots=4, chunk=2048)
        sent = [[early] + h[0][1:]] + h[1:]
        for i in range(4):
            fx[i], fy[i] = send_all(sent[i], XN), send_all(sent[i], YN)
        for i in (0, 1):
            fd[i] = send_all(fx[i], YN)
        for i in (2, 3):
            fd[i] = send_all(fy[i], XN)
        k_m, v_m = {0: k_own}, {0: v_own}
        for m in (XN, YN):
            k_m[m], v_m[m] = send(k_own, m), send(v_own, m)
        k_m[DIAG], v_m[DIAG] = send(k_m[XN], YN), send(v_m[YN], XN)
        for m in (0, XN, YN, DIAG):
            k_m[m | CORE], v_m[m | CORE] = send(k_m[m], CORE), send(v_m[m], CORE)
        keys, values = [k_m[m] for m in range(n_dev)], [v_m[m] for m in range(n_dev)]
        k_cache, v_cache = order_blocks(keys, values)

        pos_m = by_mask(positions.reshape(n_dev, 4, piece), me)
        kpos = pos_m.reshape(1, seq)
        plan = {
            U0A: [(0, 0, h[0]), (0, 1, h[1])], U0B: [(0, 2, h[2]), (0, 3, h[3])],
            U1A: [(XN, 0, fx[0]), (YN, 0, fy[0])], U1B: [(XN, 1, fx[1]), (YN, 2, fy[2])],
            U2A: [(XN, 2, fx[2]), (YN, 3, fy[3])], U2B: [(XN, 3, fx[3]), (YN, 1, fy[1])],
            U3A: [(DIAG, 0, fd[0]), (DIAG, 2, fd[2])], U3B: [(DIAG, 1, fd[1]), (DIAG, 3, fd[3])],
        }
        qpos = jnp.concatenate([pos_m[m | c, i] for u in UNITS for c in (0, CORE) for m, i, _ in plan[u]]).reshape(len(UNITS), -1)
        qpos, kpos = as_float(qpos, kpos)

        parts = {}
        for index, name in enumerate(UNITS):
            blocks = plan[name]
            mine = sum((b for _, _, b in blocks), [])
            lhs = mine + send_all(mine, CORE)
            splits = [piece] * len(blocks) + [piece * len(blocks)]
            *own, other = unit_call(lhs, wq_loc, wo_loc, keys, values, qpos, kpos, index, splits)
            back = send(other, CORE)
            for j, (m, i, _) in enumerate(blocks):
                parts[m, i] = [(own[j], 0), (back, j * piece)]

        def total(*jobs):
            return sums([(k, 0, piece, t) for k, t in enumerate(jobs)], [piece] * len(jobs))

        def both(i, j):
            px, py = total(parts[DIAG, i], parts[DIAG, j])
            return send(px, XN), send(py, YN)

        got = {}
        px, = total(parts[XN, 0])
        got[0] = send(px, XN)
        px, py = total(parts[XN, 1], parts[YN, 2])
        got[1], got[2] = send(px, XN), send(py, YN)
        py, = total(parts[YN, 3])
        got[3] = send(py, YN)
        last = []
        for i, j, cuts in ((0, 2, (piece,)), (1, 3, (piece // 2, piece // 4, piece // 4))):
            hx, hy = both(i, j)
            first = 0
            for n in cuts:
                jobs = []
                for k, (p, owner, far) in enumerate(((i, YN, hx), (j, XN, hy))):
                    jobs.append((k, 0, n, [(a, f + first) for a, f in parts[owner, p] + [(far, 0)]]))
                py, px = sums(jobs, [n, n])
                last.append((n, (i * piece + first, send(py, YN)), (j * piece + first, send(px, XN))))
                first += n
        y, = sums([(0, i * piece, piece, parts[0, i] + [(got[i], 0)]) for i in range(4)], [rows])
        for n, *arrived in last:
            y, = sums([(0, f, n, [(y, f), (a, 0)]) for f, a in arrived], [rows], into=y)
        return y, k_cache, v_cache

    return jax.shard_map(
        local_step,
        mesh=mesh,
        in_specs=(P(AXIS, None), P(None), P(None, AXIS), P(None, None), P(AXIS, None), P(None)),
        out_specs=(P(AXIS, None), P(None, None), P(None, None)),
        check_vma=False,
    )
```

```python
import functools
import math

import jax
import jax.numpy as jnp
from jax import lax
from jax.experimental import pallas as pl
from jax.experimental.pallas import tpu as pltpu
from jax.sharding import PartitionSpec as P


NORM_EPS = 1e-6
LOG2E = math.log2(math.e)
VMEM_BYTES = 67043328
NORM_BYTES = 56 << 20
AXIS = "model"
CORE, XN, YN, DIAG = 1, 2, 4, 6
BF16, F32 = jnp.bfloat16, jnp.float32


def _norm_kernel(chunk, steps, x_ref, g_ref, *out_refs, landing=((),)):
    rows, width = x_ref.shape
    n_chunks = width // chunk

    def cols(c):
        return pl.ds(pl.multiple_of(c * chunk, chunk), chunk)

    def load(c):
        return x_ref[:, cols(c)].astype(F32)

    def fold(v):
        acc = v[:, :128]
        for i in range(1, chunk // 128):
            acc = acc + v[:, i * 128:(i + 1) * 128]
        return acc

    def square(c, acc):
        d = load(c) - mean
        return acc + fold(d * d)

    zero = jnp.zeros((rows, 128), F32)
    total, part = zero, n_chunks // len(landing)
    for i, copies in enumerate(landing):
        for c in copies:
            c.wait()
        total = lax.fori_loop(i * part, (i + 1) * part, lambda c, acc: acc + fold(load(c)), total)
    mean = jnp.sum(total, axis=1, keepdims=True) / width
    rstd = lax.rsqrt(jnp.sum(lax.fori_loop(0, n_chunks, square, zero), axis=1, keepdims=True) / width + NORM_EPS)
    for i, out_ref in enumerate(out_refs):
        @pl.when(pl.program_id(0) // steps == i)
        def _():
            def put(c, _):
                out_ref[:, cols(c)] = ((load(c) - mean) * rstd * g_ref[:, cols(c)]).astype(BF16)
                return 0

            lax.fori_loop(0, n_chunks, put, 0)


def _norm_first_kernel(chunk, x_hbm, g_hbm, out_ref, x_buf, g_buf, sem):
    rows, width = x_buf.shape
    halves = [pl.ds(i * width // 2, width // 2) for i in range(2)]
    copies = [pltpu.make_async_copy(x_hbm.at[pl.ds(0, rows), c], x_buf.at[:, c], sem.at[i]) for i, c in enumerate(halves)]
    copies.append(pltpu.make_async_copy(g_hbm, g_buf, sem.at[2]))
    for c in copies:
        c.start()
    _norm_kernel(chunk, 1, x_buf, g_buf, out_ref, landing=(copies[:1], copies[1:]))


def norm_first(x, gain, rows):
    width = x.shape[1]
    hbm = pl.BlockSpec(memory_space=pltpu.HBM)
    return pl.pallas_call(
        functools.partial(_norm_first_kernel, 4608),
        grid=(1,),
        in_specs=[hbm, hbm],
        out_specs=pl.BlockSpec(memory_space=pltpu.VMEM),
        out_shape=pltpu.VMEM((rows, width), BF16),
        scratch_shapes=[pltpu.VMEM((rows, width), BF16), pltpu.VMEM(gain.shape, F32), pltpu.SemaphoreType.DMA((3,))],
        compiler_params=pltpu.CompilerParams(dimension_semantics=("arbitrary",), vmem_limit_bytes=NORM_BYTES),
        cost_estimate=pl.CostEstimate(flops=8 * rows * width, bytes_accessed=4 * rows * width, transcendentals=0),
        name="norm",
    )(x, gain)


def norm_rows(x, gain, first, piece, count, rows, stride=1):
    width = x.shape[1]
    steps = piece // rows

    def out_map(i):
        return lambda s: (jnp.clip(s - i * steps, 0, steps - 1), 0)

    return pl.pallas_call(
        functools.partial(_norm_kernel, 2048, steps),
        grid=(count * steps,),
        in_specs=[pl.BlockSpec((rows, width), lambda s: (first // rows + stride * s, 0)), pl.BlockSpec((1, width), lambda s: (0, 0))],
        out_specs=[pl.BlockSpec((rows, width), out_map(i)) for i in range(count)],
        out_shape=[jax.ShapeDtypeStruct((piece, width), BF16)] * count,
        compiler_params=pltpu.CompilerParams(dimension_semantics=("arbitrary",), vmem_limit_bytes=NORM_BYTES),
        cost_estimate=pl.CostEstimate(flops=8 * count * piece * width, bytes_accessed=4 * count * piece * width, transcendentals=0),
        name="norm",
    )(x, gain)


def _order_kernel(n, *refs):
    me = lax.axis_index(AXIS)
    k_out, v_out = refs[2 * n:]
    for m, (top, rest) in enumerate(zip(refs[:n], refs[n:2 * n])):
        high, rows = top.shape[0], (top.shape[0] + rest.shape[0]) // 2
        first = pl.multiple_of((me ^ m) * rows, rows)
        k_out[pl.ds(first, high), :] = top[...]
        k_out[pl.ds(pl.multiple_of(first + high, 16), rows - high), :] = rest[rows:, :]
        v_out[pl.ds(first, rows), :] = rest[:rows, :]


def order_blocks(tops, rests):
    n, cols = len(tops), tops[0].shape[1]
    rows = (tops[0].shape[0] + rests[0].shape[0]) // 2
    return pl.pallas_call(
        functools.partial(_order_kernel, n),
        in_specs=[pl.BlockSpec(memory_space=pltpu.VMEM)] * (2 * n),
        out_specs=[pl.BlockSpec(memory_space=pltpu.VMEM)] * 2,
        out_shape=[jax.ShapeDtypeStruct((rows * n, cols), BF16)] * 2,
        cost_estimate=pl.CostEstimate(flops=2 * rows * n * cols, bytes_accessed=8 * rows * n * cols, transcendentals=0),
        name="order",
    )(*tops, *rests)


def _unit_kernel(names, parts, n_lhs, n_out, index, *flat):
    r = dict(zip(names, flat))
    lhs = [r[f"lhs{i}"] for i in range(n_lhs)]
    outs = [r[f"out{i}"] for i in range(n_out)]
    ring, ring_sem, q_buf = r["ring"], r["ring_sem"], r["q_buf"]
    slots, chunk = ring.shape[:2]
    do_q, do_o = "q" in parts, "o" in parts
    rows, proj = q_buf.shape
    n_q = r["wq"].shape[0] // chunk if do_q else 0
    n_o = r["wo"].shape[1] // chunk if do_o else 0
    total = n_q + n_o

    def at(i):
        return pl.ds(pl.multiple_of(i * chunk, chunk), chunk)

    def wq_copy(i, slot):
        return pltpu.make_async_copy(r["wq"].at[at(i), :], ring.at[slot], ring_sem.at[slot])

    def wo_copy(i, slot):
        return pltpu.make_async_copy(r["wo"].at[:, at(i - n_q)], ring.at[slot], ring_sem.at[slot])

    def h_copies(i, slot):
        cps, first = [], 0
        for j, h in enumerate(lhs):
            n = h.shape[0]
            cps.append(pltpu.make_async_copy(h.at[:, at(i)], r["h_buf"].at[slot, pl.ds(first, n), :], r["h_sem"].at[slot, j]))
            first += n
        return cps

    def y_copies(i, slot):
        cps, first = [], 0
        for j, out in enumerate(outs):
            n = out.shape[0]
            cps.append(pltpu.make_async_copy(r["y_buf"].at[slot, pl.ds(first, n), :], out.at[:, at(i)], r["y_sem"].at[slot, j]))
            first += n
        return cps

    def fetch(i, slot):
        if do_q:
            @pl.when(i < n_q)
            def _():
                wq_copy(i, slot).start()
                for c in h_copies(i, slot):
                    c.start()
        if do_o:
            @pl.when((i >= n_q) & (i < total))
            def _():
                wo_copy(i, slot).start()

    for i in range(slots):
        if i < n_q:
            wq_copy(i, i).start()
            for c in h_copies(i, i):
                c.start()
        elif i < total:
            wo_copy(i, i).start()
    extra = []
    if do_o:
        row, col = (lax.broadcasted_iota(jnp.int32, (rows, rows), d) for d in (0, 1))
        mine = jnp.where(row == col, r["qpos"][index:index + 1, :], 0.0)
        r["q_col"][...] = jnp.sum(mine, axis=1, keepdims=True)
        for m in range(r["kv_sem"].shape[0]):
            top, rest = r[f"k{m}"], r[f"v{m}"]
            high, n = top.shape[0], (top.shape[0] + rest.shape[0]) // 2
            moves = ((top, 0, high, "k_buf", 0), (rest, n, n - high, "k_buf", high), (rest, 0, n, "v_buf", 0))
            for j, (src, first, count, buf, to) in enumerate(moves):
                extra.append(pltpu.make_async_copy(src.at[pl.ds(first, count), :], r[buf].at[pl.ds(m * n + to, count), :], r["kv_sem"].at[m, j]))
    for c in extra:
        c.start()

    if do_q:
        acc = r["acc"]
        acc[...] = jnp.zeros_like(acc)

        def q_step(i, _):
            slot = lax.rem(i, slots)
            wq_copy(i, slot).wait()
            for c in h_copies(i, slot):
                c.wait()
            acc[...] += jnp.dot(r["h_buf"][slot], ring[slot], preferred_element_type=F32)
            fetch(i + slots, slot)
            return 0

        lax.fori_loop(0, n_q, q_step, 0)
        if not do_o:
            high, cols = outs[0].shape
            outs[0][...] = acc[:high, :cols].astype(BF16)
            outs[1][:rows, :] = acc[:, cols:].astype(BF16)
            outs[1][rows:, :] = acc[high:, :cols].astype(BF16)
            return
        q_buf[...] = acc[...].astype(BF16)

    for c in extra:
        c.wait()
    k_buf, v_buf, o_buf, y_buf = r["k_buf"], r["v_buf"], r["o_buf"], r["y_buf"]
    head = k_buf.shape[1]
    heads = proj // head

    half = rows // 2

    def score(s_ref, n, b):
        cols = pl.ds(pl.multiple_of(n * head, head), head)
        s_ref[...] = lax.dot_general(q_buf[pl.ds(b * half, half), cols], k_buf[...], (((1,), (1,)), ((), ())), preferred_element_type=F32)

    def attend(s_ref, n, b):
        mine, cols = pl.ds(b * half, half), pl.ds(pl.multiple_of(n * head, head), head)
        s = jnp.where(r["kpos"][...] <= r["q_col"][mine, :], s_ref[...], -1e30)
        e = jnp.exp2((s - jnp.max(s, axis=-1, keepdims=True)) * (head ** -0.5 * LOG2E))
        p = (e * (1.0 / jnp.sum(e, axis=-1, keepdims=True))).astype(BF16)
        o_buf[mine, cols] = jnp.dot(p, v_buf[...], preferred_element_type=F32).astype(BF16)

    def one_head(n, _):
        score(r["s_b"], n, 1)
        attend(r["s_a"], n, 0)
        score(r["s_a"], jnp.minimum(n + 1, heads - 1), 0)
        attend(r["s_b"], n, 1)
        return 0

    score(r["s_a"], 0, 0)
    lax.fori_loop(0, heads, one_head, 0)

    def o_step(i, _):
        slot, yslot = lax.rem(n_q + i, slots), lax.rem(i, 2)
        wo_copy(n_q + i, slot).wait()

        @pl.when(i >= 2)
        def _():
            for c in y_copies(i - 2, yslot):
                c.wait()

        y_buf[yslot] = jnp.dot(o_buf[...], ring[slot], preferred_element_type=F32).astype(BF16)
        for c in y_copies(i, yslot):
            c.start()
        fetch(n_q + i + slots, slot)
        return 0

    lax.fori_loop(0, n_o, o_step, 0)
    for i in (n_o - 2, n_o - 1):
        for c in y_copies(i, i % 2):
            c.wait()


def unit_call(lhs, wq, wo, keys, values, qpos, kpos, index, splits, slots=7, chunk=None):
    parts = ("q" if wq is not None else "") + ("o" if wo is not None else "")
    rows = sum(h.shape[0] for h in lhs)
    proj = wq.shape[1]
    width = wq.shape[0]
    chunk = chunk or proj
    any_ = pl.BlockSpec(memory_space=pl.ANY)
    ins = [(f"lhs{i}", h, any_) for i, h in enumerate(lhs)]
    scratch = [("ring", pltpu.VMEM((slots, chunk, proj), BF16)), ("ring_sem", pltpu.SemaphoreType.DMA((slots,))), ("q_buf", pltpu.VMEM((rows, proj), BF16))]
    flops, moved = 0, 0
    if wq is not None:
        ins.append(("wq", wq, any_))
        scratch += [("h_buf", pltpu.VMEM((slots, rows, chunk), BF16)), ("h_sem", pltpu.SemaphoreType.DMA((slots, len(lhs)))), ("acc", pltpu.VMEM((rows, proj), F32))]
        flops += 2 * rows * proj * width
        moved += 2 * (rows + proj) * width
    if wo is not None:
        n_keys, head = kpos.shape[1], keys[0].shape[1]
        ins.append(("wo", wo, any_))
        ins += [(f"k{m}", k, any_) for m, k in enumerate(keys)] + [(f"v{m}", v, any_) for m, v in enumerate(values)]
        ins += [("qpos", qpos, pl.BlockSpec(qpos.shape, lambda i: (0, 0))), ("kpos", kpos, pl.BlockSpec((1, n_keys), lambda i: (0, 0)))]
        scratch += [
            ("o_buf", pltpu.VMEM((rows, proj), BF16)), ("y_buf", pltpu.VMEM((2, rows, chunk), BF16)), ("y_sem", pltpu.SemaphoreType.DMA((2, len(splits)))),
            ("q_col", pltpu.VMEM((rows, 1), F32)), ("s_a", pltpu.VMEM((rows // 2, n_keys), F32)), ("s_b", pltpu.VMEM((rows // 2, n_keys), F32)),
            ("k_buf", pltpu.VMEM((n_keys, head), BF16)), ("v_buf", pltpu.VMEM((n_keys, head), BF16)), ("kv_sem", pltpu.SemaphoreType.DMA((len(keys), 3))),
        ]
        flops += 2 * rows * proj * (width + 2 * n_keys)
        moved += 2 * (rows + proj) * width
        outs = [((n, width), any_) for n in splits]
    else:
        outs = [((n, proj // 2), pl.BlockSpec((n, proj // 2), lambda i: (0, 0))) for n in splits]
    names = [i[0] for i in ins] + [f"out{i}" for i in range(len(outs))] + [s[0] for s in scratch]
    res = pl.pallas_call(
        functools.partial(_unit_kernel, names, parts, len(lhs), len(outs), index),
        grid=(1,),
        in_specs=[i[2] for i in ins],
        out_specs=[o[1] for o in outs],
        out_shape=[jax.ShapeDtypeStruct(o[0], BF16) for o in outs],
        scratch_shapes=[s[1] for s in scratch],
        compiler_params=pltpu.CompilerParams(dimension_semantics=("arbitrary",), vmem_limit_bytes=VMEM_BYTES if wo is not None else NORM_BYTES),
        cost_estimate=pl.CostEstimate(flops=flops, bytes_accessed=moved, transcendentals=0),
    )(*[i[1] for i in ins])
    return res


def _sums_kernel(jobs, n_in, *refs):
    ins, outs, bufs, in_sem, out_sem = refs[:n_in], refs[n_in:-3], refs[-3], refs[-2], refs[-1]
    halves = in_sem.shape[0]
    width = bufs.shape[1] // halves
    loads, stores, slots = {}, [], []
    at = 0
    for out, first, rows, terms in jobs:
        slots.append([])
        for _ in terms:
            slots[-1].append(at)
            at += rows
    n = 0
    for c in range(halves):
        cols = pl.ds(c * width, width)
        n = 0
        for j, (_, _, rows, terms) in enumerate(jobs):
            for i, (ref, first) in enumerate(terms):
                loads[c, j, i] = pltpu.make_async_copy(ins[ref].at[pl.ds(first, rows), cols], bufs.at[pl.ds(slots[j][i], rows), cols], in_sem.at[c, n])
                loads[c, j, i].start()
                n += 1
    for c in range(halves):
        for j, (out, first, rows, terms) in enumerate(jobs):
            for i in range(len(terms)):
                loads[c, j, i].wait()

            def some(k, _):
                cols = pl.ds(pl.multiple_of(c * width + k * 512, 512), 512)
                total = bufs[pl.ds(slots[j][0], rows), cols].astype(F32)
                for at in slots[j][1:]:
                    total = total + bufs[pl.ds(at, rows), cols].astype(F32)
                bufs[pl.ds(slots[j][0], rows), cols] = total.astype(BF16)
                return 0

            lax.fori_loop(0, width // 512, some, 0)
            cols = pl.ds(c * width, width)
            stores.append(pltpu.make_async_copy(bufs.at[pl.ds(slots[j][0], rows), cols], outs[out].at[pl.ds(first, rows), cols], out_sem.at[c, j]))
            stores[-1].start()
    for c in stores:
        c.wait()


def sums(jobs, out_rows, into=None):
    arrays = [] if into is None else [into]
    spec = []
    for out, first, rows, terms in jobs:
        at = []
        for a, f in terms:
            k = next((k for k, b in enumerate(arrays) if b is a), len(arrays))
            if k == len(arrays):
                arrays.append(a)
            at.append((k, f))
        spec.append((out, first, rows, tuple(at)))
    width = arrays[0].shape[1]
    n_terms = sum(len(j[3]) for j in jobs)
    rows_in = sum(j[2] * len(j[3]) for j in jobs)
    cuts = 1 if rows_in <= 32 else 2
    any_ = pl.BlockSpec(memory_space=pl.ANY)
    return pl.pallas_call(
        functools.partial(_sums_kernel, tuple(spec), len(arrays)),
        in_specs=[any_] * len(arrays),
        out_specs=[any_] * len(out_rows),
        out_shape=[jax.ShapeDtypeStruct((r, width), BF16) for r in out_rows],
        input_output_aliases={} if into is None else {0: 0},
        scratch_shapes=[pltpu.VMEM((rows_in, width), BF16), pltpu.SemaphoreType.DMA((cuts, n_terms)), pltpu.SemaphoreType.DMA((cuts, len(jobs)))],
        compiler_params=pltpu.CompilerParams(vmem_limit_bytes=VMEM_BYTES),
        cost_estimate=pl.CostEstimate(flops=rows_in * width, bytes_accessed=4 * rows_in * width, transcendentals=0),
        name="sums",
    )(*arrays)


def _where_kernel(q_ref, k_ref, q_out, k_out):
    q_out[...] = q_ref[...].astype(F32)
    k_out[...] = k_ref[...].astype(F32)


def as_float(q, k):
    return pl.pallas_call(
        _where_kernel,
        in_specs=[pl.BlockSpec(memory_space=pltpu.VMEM)] * 2,
        out_specs=[pl.BlockSpec(memory_space=pltpu.VMEM)] * 2,
        out_shape=[jax.ShapeDtypeStruct(q.shape, F32), jax.ShapeDtypeStruct(k.shape, F32)],
        cost_estimate=pl.CostEstimate(flops=q.size, bytes_accessed=16 * q.size, transcendentals=0),
        name="where",
    )(q, k)


CUTS = (16, 32, 16)
UNITS = U1A, U1B, U2A, U2B, U3A, U3B, U0A, U0B = ("u1a", "u1b", "u2a", "u2b", "u3a", "u3b", "u0a", "u0b")


def solution(mesh):
    n_dev = mesh.shape[AXIS]

    def send(value, mask):
        return lax.ppermute(value, AXIS, [(i, i ^ mask) for i in range(n_dev)])

    def by_mask(arr, me):
        cube = arr.reshape((2, 2, 2) + arr.shape[1:])
        for axis, bit in ((0, 4), (1, 2), (2, 1)):
            cube = jnp.where((me & bit) != 0, jnp.flip(cube, axis), cube)
        return cube.reshape(arr.shape)

    def local_step(x_loc, ln_gain, wq_loc, w_kv, wo_loc, positions):
        me = lax.axis_index(AXIS)
        rows, width = x_loc.shape
        seq = positions.shape[0]
        piece = rows // 4
        gain = ln_gain.reshape(1, width)

        def send_all(values, mask):
            return [send(v, mask) for v in values]

        h, fx, fy, fd = [[] for _ in range(4)], [None] * 4, [None] * 4, [None] * 4
        a, b, _ = CUTS
        early = norm_first(x_loc, gain, a)
        middle, = norm_rows(x_loc, gain, a, b, 1, a)
        head_rows, tail_rows = norm_rows(x_loc, gain, 0, a, 2, a, (a + b) // a)
        h[0] = [head_rows, middle, tail_rows]
        for i, v in enumerate(norm_rows(x_loc, gain, piece, piece, 3, piece // 2)):
            h[i + 1].append(v)
        k_own, v_own = unit_call(sum(h, []), w_kv, None, None, None, None, None, 0, [rows - piece, rows + piece], slots=4, chunk=2048)
        sent = [[early] + h[0][1:]] + h[1:]
        for i in range(4):
            fx[i], fy[i] = send_all(sent[i], XN), send_all(sent[i], YN)
        for i in (0, 1):
            fd[i] = send_all(fx[i], YN)
        for i in (2, 3):
            fd[i] = send_all(fy[i], XN)
        k_m, v_m = {0: k_own}, {0: v_own}
        for m in (XN, YN):
            k_m[m], v_m[m] = send(k_own, m), send(v_own, m)
        k_m[DIAG], v_m[DIAG] = send(k_m[XN], YN), send(v_m[YN], XN)
        for m in (0, XN, YN, DIAG):
            k_m[m | CORE], v_m[m | CORE] = send(k_m[m], CORE), send(v_m[m], CORE)
        keys, values = [k_m[m] for m in range(n_dev)], [v_m[m] for m in range(n_dev)]
        k_cache, v_cache = order_blocks(keys, values)

        pos_m = by_mask(positions.reshape(n_dev, 4, piece), me)
        kpos = pos_m.reshape(1, seq)
        plan = {
            U0A: [(0, 0, h[0]), (0, 1, h[1])], U0B: [(0, 2, h[2]), (0, 3, h[3])],
            U1A: [(XN, 0, fx[0]), (YN, 0, fy[0])], U1B: [(XN, 1, fx[1]), (YN, 2, fy[2])],
            U2A: [(XN, 2, fx[2]), (YN, 3, fy[3])], U2B: [(XN, 3, fx[3]), (YN, 1, fy[1])],
            U3A: [(DIAG, 0, fd[0]), (DIAG, 2, fd[2])], U3B: [(DIAG, 1, fd[1]), (DIAG, 3, fd[3])],
        }
        qpos = jnp.concatenate([pos_m[m | c, i] for u in UNITS for c in (0, CORE) for m, i, _ in plan[u]]).reshape(len(UNITS), -1)
        qpos, kpos = as_float(qpos, kpos)

        parts = {}
        for index, name in enumerate(UNITS):
            blocks = plan[name]
            mine = sum((b for _, _, b in blocks), [])
            lhs = mine + send_all(mine, CORE)
            splits = [piece] * len(blocks) + [piece * len(blocks)]
            *own, other = unit_call(lhs, wq_loc, wo_loc, keys, values, qpos, kpos, index, splits)
            back = send(other, CORE)
            for j, (m, i, _) in enumerate(blocks):
                parts[m, i] = [(own[j], 0), (back, j * piece)]

        def total(*jobs):
            return sums([(k, 0, piece, t) for k, t in enumerate(jobs)], [piece] * len(jobs))

        def both(i, j):
            px, py = total(parts[DIAG, i], parts[DIAG, j])
            return send(px, XN), send(py, YN)

        got = {}
        px, = total(parts[XN, 0])
        got[0] = send(px, XN)
        px, py = total(parts[XN, 1], parts[YN, 2])
        got[1], got[2] = send(px, XN), send(py, YN)
        py, = total(parts[YN, 3])
        got[3] = send(py, YN)
        last = []
        for i, j, cuts in ((0, 2, (piece,)), (1, 3, (piece // 2, piece // 4, piece // 8, piece // 8))):
            hx, hy = both(i, j)
            first = 0
            for n in cuts:
                jobs = []
                for k, (p, owner, far) in enumerate(((i, YN, hx), (j, XN, hy))):
                    jobs.append((k, 0, n, [(a, f + first) for a, f in parts[owner, p] + [(far, 0)]]))
                py, px = sums(jobs, [n, n])
                last.append((n, (i * piece + first, send(py, YN)), (j * piece + first, send(px, XN))))
                first += n
        y, = sums([(0, i * piece, piece, parts[0, i] + [(got[i], 0)]) for i in range(4)], [rows])
        for n, *arrived in last:
            y, = sums([(0, f, n, [(y, f), (a, 0)]) for f, a in arrived], [rows], into=y)
        return y, k_cache, v_cache

    return jax.shard_map(
        local_step,
        mesh=mesh,
        in_specs=(P(AXIS, None), P(None), P(None, AXIS), P(None, None), P(AXIS, None), P(None)),
        out_specs=(P(AXIS, None), P(None, None), P(None, None)),
        check_vma=False,
    )
```

```python
import functools
import math

import jax
import jax.numpy as jnp
from jax import lax
from jax.experimental import pallas as pl
from jax.experimental.pallas import tpu as pltpu
from jax.sharding import PartitionSpec as P


NORM_EPS = 1e-6
LOG2E = math.log2(math.e)
VMEM_BYTES = 67043328
NORM_BYTES = 56 << 20
AXIS = "model"
CORE, XN, YN, DIAG = 1, 2, 4, 6
BF16, F32 = jnp.bfloat16, jnp.float32


def _norm_kernel(chunk, steps, x_ref, g_ref, *out_refs):
    rows, width = x_ref.shape
    n_chunks = width // chunk

    def cols(c):
        return pl.ds(pl.multiple_of(c * chunk, chunk), chunk)

    def load(c):
        return x_ref[:, cols(c)].astype(F32)

    def fold(v):
        acc = v[:, :128]
        for i in range(1, chunk // 128):
            acc = acc + v[:, i * 128:(i + 1) * 128]
        return acc

    def square(c, acc):
        d = load(c) - mean
        return acc + fold(d * d)

    zero = jnp.zeros((rows, 128), F32)
    mean = jnp.sum(lax.fori_loop(0, n_chunks, lambda c, acc: acc + fold(load(c)), zero), axis=1, keepdims=True) / width
    rstd = lax.rsqrt(jnp.sum(lax.fori_loop(0, n_chunks, square, zero), axis=1, keepdims=True) / width + NORM_EPS)
    for i, out_ref in enumerate(out_refs):
        @pl.when(pl.program_id(0) // steps == i)
        def _():
            def put(c, _):
                out_ref[:, cols(c)] = ((load(c) - mean) * rstd * g_ref[:, cols(c)]).astype(BF16)
                return 0

            lax.fori_loop(0, n_chunks, put, 0)


def _fetch_kernel(x_hbm, out_ref, sem):
    copy = pltpu.make_async_copy(x_hbm.at[pl.ds(0, out_ref.shape[0]), :], out_ref, sem)
    copy.start()
    copy.wait()


def fetch_first(x, rows):
    return pl.pallas_call(
        _fetch_kernel,
        in_specs=[pl.BlockSpec(memory_space=pltpu.HBM)],
        out_specs=pl.BlockSpec(memory_space=pltpu.VMEM),
        out_shape=pltpu.VMEM((rows, x.shape[1]), BF16),
        scratch_shapes=[pltpu.SemaphoreType.DMA],
        compiler_params=pltpu.CompilerParams(vmem_limit_bytes=NORM_BYTES),
        cost_estimate=pl.CostEstimate(flops=rows * x.shape[1], bytes_accessed=4 * rows * x.shape[1], transcendentals=0),
        name="fetch",
    )(x)


def norm_rows(x, gain, first, piece, count, rows, stride=1):
    width = x.shape[1]
    steps = piece // rows

    def out_map(i):
        return lambda s: (jnp.clip(s - i * steps, 0, steps - 1), 0)

    return pl.pallas_call(
        functools.partial(_norm_kernel, 2048, steps),
        grid=(count * steps,),
        in_specs=[pl.BlockSpec((rows, width), lambda s: (first // rows + stride * s, 0)), pl.BlockSpec((1, width), lambda s: (0, 0))],
        out_specs=[pl.BlockSpec((rows, width), out_map(i)) for i in range(count)],
        out_shape=[jax.ShapeDtypeStruct((piece, width), BF16)] * count,
        compiler_params=pltpu.CompilerParams(dimension_semantics=("arbitrary",), vmem_limit_bytes=NORM_BYTES),
        cost_estimate=pl.CostEstimate(flops=8 * count * piece * width, bytes_accessed=4 * count * piece * width, transcendentals=0),
        name="norm",
    )(x, gain)


def _order_kernel(n, *refs):
    me = lax.axis_index(AXIS)
    k_out, v_out = refs[2 * n:]
    for m, (top, rest) in enumerate(zip(refs[:n], refs[n:2 * n])):
        high, rows = top.shape[0], (top.shape[0] + rest.shape[0]) // 2
        first = pl.multiple_of((me ^ m) * rows, rows)
        k_out[pl.ds(first, high), :] = top[...]
        k_out[pl.ds(pl.multiple_of(first + high, 16), rows - high), :] = rest[rows:, :]
        v_out[pl.ds(first, rows), :] = rest[:rows, :]


def order_blocks(tops, rests):
    n, cols = len(tops), tops[0].shape[1]
    rows = (tops[0].shape[0] + rests[0].shape[0]) // 2
    return pl.pallas_call(
        functools.partial(_order_kernel, n),
        in_specs=[pl.BlockSpec(memory_space=pltpu.VMEM)] * (2 * n),
        out_specs=[pl.BlockSpec(memory_space=pltpu.VMEM)] * 2,
        out_shape=[jax.ShapeDtypeStruct((rows * n, cols), BF16)] * 2,
        cost_estimate=pl.CostEstimate(flops=2 * rows * n * cols, bytes_accessed=8 * rows * n * cols, transcendentals=0),
        name="order",
    )(*tops, *rests)


def _unit_kernel(names, parts, n_lhs, n_out, index, *flat):
    r = dict(zip(names, flat))
    lhs = [r[f"lhs{i}"] for i in range(n_lhs)]
    outs = [r[f"out{i}"] for i in range(n_out)]
    ring, ring_sem, q_buf = r["ring"], r["ring_sem"], r["q_buf"]
    slots, chunk = ring.shape[:2]
    do_q, do_o = "q" in parts, "o" in parts
    rows, proj = q_buf.shape
    n_q = r["wq"].shape[0] // chunk if do_q else 0
    n_o = r["wo"].shape[1] // chunk if do_o else 0
    total = n_q + n_o

    def at(i):
        return pl.ds(pl.multiple_of(i * chunk, chunk), chunk)

    def wq_copy(i, slot):
        return pltpu.make_async_copy(r["wq"].at[at(i), :], ring.at[slot], ring_sem.at[slot])

    def wo_copy(i, slot):
        return pltpu.make_async_copy(r["wo"].at[:, at(i - n_q)], ring.at[slot], ring_sem.at[slot])

    def h_copies(i, slot):
        cps, first = [], 0
        for j, h in enumerate(lhs):
            n = h.shape[0]
            cps.append(pltpu.make_async_copy(h.at[:, at(i)], r["h_buf"].at[slot, pl.ds(first, n), :], r["h_sem"].at[slot, j]))
            first += n
        return cps

    def y_copies(i, slot):
        cps, first = [], 0
        for j, out in enumerate(outs):
            n = out.shape[0]
            cps.append(pltpu.make_async_copy(r["y_buf"].at[slot, pl.ds(first, n), :], out.at[:, at(i)], r["y_sem"].at[slot, j]))
            first += n
        return cps

    def fetch(i, slot):
        if do_q:
            @pl.when(i < n_q)
            def _():
                wq_copy(i, slot).start()
                for c in h_copies(i, slot):
                    c.start()
        if do_o:
            @pl.when((i >= n_q) & (i < total))
            def _():
                wo_copy(i, slot).start()

    for i in range(slots):
        if i < n_q:
            wq_copy(i, i).start()
            for c in h_copies(i, i):
                c.start()
        elif i < total:
            wo_copy(i, i).start()
    extra = []
    if do_o:
        row, col = (lax.broadcasted_iota(jnp.int32, (rows, rows), d) for d in (0, 1))
        mine = jnp.where(row == col, r["qpos"][index:index + 1, :], 0.0)
        r["q_col"][...] = jnp.sum(mine, axis=1, keepdims=True)
        for m in range(r["kv_sem"].shape[0]):
            top, rest = r[f"k{m}"], r[f"v{m}"]
            high, n = top.shape[0], (top.shape[0] + rest.shape[0]) // 2
            moves = ((top, 0, high, "k_buf", 0), (rest, n, n - high, "k_buf", high), (rest, 0, n, "v_buf", 0))
            for j, (src, first, count, buf, to) in enumerate(moves):
                extra.append(pltpu.make_async_copy(src.at[pl.ds(first, count), :], r[buf].at[pl.ds(m * n + to, count), :], r["kv_sem"].at[m, j]))
    for c in extra:
        c.start()

    if do_q:
        acc = r["acc"]
        acc[...] = jnp.zeros_like(acc)

        def q_step(i, _):
            slot = lax.rem(i, slots)
            wq_copy(i, slot).wait()
            for c in h_copies(i, slot):
                c.wait()
            acc[...] += jnp.dot(r["h_buf"][slot], ring[slot], preferred_element_type=F32)
            fetch(i + slots, slot)
            return 0

        lax.fori_loop(0, n_q, q_step, 0)
        if not do_o:
            high, cols = outs[0].shape
            outs[0][...] = acc[:high, :cols].astype(BF16)
            outs[1][:rows, :] = acc[:, cols:].astype(BF16)
            outs[1][rows:, :] = acc[high:, :cols].astype(BF16)
            return
        q_buf[...] = acc[...].astype(BF16)

    for c in extra:
        c.wait()
    k_buf, v_buf, o_buf, y_buf = r["k_buf"], r["v_buf"], r["o_buf"], r["y_buf"]
    head = k_buf.shape[1]
    heads = proj // head

    half = rows // 2

    def score(s_ref, n, b):
        cols = pl.ds(pl.multiple_of(n * head, head), head)
        s_ref[...] = lax.dot_general(q_buf[pl.ds(b * half, half), cols], k_buf[...], (((1,), (1,)), ((), ())), preferred_element_type=F32)

    def attend(s_ref, n, b):
        mine, cols = pl.ds(b * half, half), pl.ds(pl.multiple_of(n * head, head), head)
        s = jnp.where(r["kpos"][...] <= r["q_col"][mine, :], s_ref[...], -1e30)
        e = jnp.exp2((s - jnp.max(s, axis=-1, keepdims=True)) * (head ** -0.5 * LOG2E))
        p = (e * (1.0 / jnp.sum(e, axis=-1, keepdims=True))).astype(BF16)
        o_buf[mine, cols] = jnp.dot(p, v_buf[...], preferred_element_type=F32).astype(BF16)

    def one_head(n, _):
        score(r["s_b"], n, 1)
        attend(r["s_a"], n, 0)
        score(r["s_a"], jnp.minimum(n + 1, heads - 1), 0)
        attend(r["s_b"], n, 1)
        return 0

    score(r["s_a"], 0, 0)
    lax.fori_loop(0, heads, one_head, 0)

    def o_step(i, _):
        slot, yslot = lax.rem(n_q + i, slots), lax.rem(i, 2)
        wo_copy(n_q + i, slot).wait()

        @pl.when(i >= 2)
        def _():
            for c in y_copies(i - 2, yslot):
                c.wait()

        y_buf[yslot] = jnp.dot(o_buf[...], ring[slot], preferred_element_type=F32).astype(BF16)
        for c in y_copies(i, yslot):
            c.start()
        fetch(n_q + i + slots, slot)
        return 0

    lax.fori_loop(0, n_o, o_step, 0)
    for i in (n_o - 2, n_o - 1):
        for c in y_copies(i, i % 2):
            c.wait()


def unit_call(lhs, wq, wo, keys, values, qpos, kpos, index, splits, slots=7, chunk=None):
    parts = ("q" if wq is not None else "") + ("o" if wo is not None else "")
    rows = sum(h.shape[0] for h in lhs)
    proj = wq.shape[1]
    width = wq.shape[0]
    chunk = chunk or proj
    any_ = pl.BlockSpec(memory_space=pl.ANY)
    ins = [(f"lhs{i}", h, any_) for i, h in enumerate(lhs)]
    scratch = [("ring", pltpu.VMEM((slots, chunk, proj), BF16)), ("ring_sem", pltpu.SemaphoreType.DMA((slots,))), ("q_buf", pltpu.VMEM((rows, proj), BF16))]
    flops, moved = 0, 0
    if wq is not None:
        ins.append(("wq", wq, any_))
        scratch += [("h_buf", pltpu.VMEM((slots, rows, chunk), BF16)), ("h_sem", pltpu.SemaphoreType.DMA((slots, len(lhs)))), ("acc", pltpu.VMEM((rows, proj), F32))]
        flops += 2 * rows * proj * width
        moved += 2 * (rows + proj) * width
    if wo is not None:
        n_keys, head = kpos.shape[1], keys[0].shape[1]
        ins.append(("wo", wo, any_))
        ins += [(f"k{m}", k, any_) for m, k in enumerate(keys)] + [(f"v{m}", v, any_) for m, v in enumerate(values)]
        ins += [("qpos", qpos, pl.BlockSpec(qpos.shape, lambda i: (0, 0))), ("kpos", kpos, pl.BlockSpec((1, n_keys), lambda i: (0, 0)))]
        scratch += [
            ("o_buf", pltpu.VMEM((rows, proj), BF16)), ("y_buf", pltpu.VMEM((2, rows, chunk), BF16)), ("y_sem", pltpu.SemaphoreType.DMA((2, len(splits)))),
            ("q_col", pltpu.VMEM((rows, 1), F32)), ("s_a", pltpu.VMEM((rows // 2, n_keys), F32)), ("s_b", pltpu.VMEM((rows // 2, n_keys), F32)),
            ("k_buf", pltpu.VMEM((n_keys, head), BF16)), ("v_buf", pltpu.VMEM((n_keys, head), BF16)), ("kv_sem", pltpu.SemaphoreType.DMA((len(keys), 3))),
        ]
        flops += 2 * rows * proj * (width + 2 * n_keys)
        moved += 2 * (rows + proj) * width
        outs = [((n, width), any_) for n in splits]
    else:
        outs = [((n, proj // 2), pl.BlockSpec((n, proj // 2), lambda i: (0, 0))) for n in splits]
    names = [i[0] for i in ins] + [f"out{i}" for i in range(len(outs))] + [s[0] for s in scratch]
    res = pl.pallas_call(
        functools.partial(_unit_kernel, names, parts, len(lhs), len(outs), index),
        grid=(1,),
        in_specs=[i[2] for i in ins],
        out_specs=[o[1] for o in outs],
        out_shape=[jax.ShapeDtypeStruct(o[0], BF16) for o in outs],
        scratch_shapes=[s[1] for s in scratch],
        compiler_params=pltpu.CompilerParams(dimension_semantics=("arbitrary",), vmem_limit_bytes=VMEM_BYTES if wo is not None else NORM_BYTES),
        cost_estimate=pl.CostEstimate(flops=flops, bytes_accessed=moved, transcendentals=0),
    )(*[i[1] for i in ins])
    return res


def _sums_kernel(jobs, n_in, *refs):
    ins, outs, bufs, in_sem, out_sem = refs[:n_in], refs[n_in:-3], refs[-3], refs[-2], refs[-1]
    halves = in_sem.shape[0]
    width = bufs.shape[1] // halves
    loads, stores, slots = {}, [], []
    at = 0
    for out, first, rows, terms in jobs:
        slots.append([])
        for _ in terms:
            slots[-1].append(at)
            at += rows
    n = 0
    for c in range(halves):
        cols = pl.ds(c * width, width)
        n = 0
        for j, (_, _, rows, terms) in enumerate(jobs):
            for i, (ref, first) in enumerate(terms):
                loads[c, j, i] = pltpu.make_async_copy(ins[ref].at[pl.ds(first, rows), cols], bufs.at[pl.ds(slots[j][i], rows), cols], in_sem.at[c, n])
                loads[c, j, i].start()
                n += 1
    for c in range(halves):
        for j, (out, first, rows, terms) in enumerate(jobs):
            for i in range(len(terms)):
                loads[c, j, i].wait()

            def some(k, _):
                cols = pl.ds(pl.multiple_of(c * width + k * 512, 512), 512)
                total = bufs[pl.ds(slots[j][0], rows), cols].astype(F32)
                for at in slots[j][1:]:
                    total = total + bufs[pl.ds(at, rows), cols].astype(F32)
                bufs[pl.ds(slots[j][0], rows), cols] = total.astype(BF16)
                return 0

            lax.fori_loop(0, width // 512, some, 0)
            cols = pl.ds(c * width, width)
            stores.append(pltpu.make_async_copy(bufs.at[pl.ds(slots[j][0], rows), cols], outs[out].at[pl.ds(first, rows), cols], out_sem.at[c, j]))
            stores[-1].start()
    for c in stores:
        c.wait()


def sums(jobs, out_rows, into=None):
    arrays = [] if into is None else [into]
    spec = []
    for out, first, rows, terms in jobs:
        at = []
        for a, f in terms:
            k = next((k for k, b in enumerate(arrays) if b is a), len(arrays))
            if k == len(arrays):
                arrays.append(a)
            at.append((k, f))
        spec.append((out, first, rows, tuple(at)))
    width = arrays[0].shape[1]
    n_terms = sum(len(j[3]) for j in jobs)
    rows_in = sum(j[2] * len(j[3]) for j in jobs)
    cuts = 1 if rows_in <= 32 else 2
    any_ = pl.BlockSpec(memory_space=pl.ANY)
    return pl.pallas_call(
        functools.partial(_sums_kernel, tuple(spec), len(arrays)),
        in_specs=[any_] * len(arrays),
        out_specs=[any_] * len(out_rows),
        out_shape=[jax.ShapeDtypeStruct((r, width), BF16) for r in out_rows],
        input_output_aliases={} if into is None else {0: 0},
        scratch_shapes=[pltpu.VMEM((rows_in, width), BF16), pltpu.SemaphoreType.DMA((cuts, n_terms)), pltpu.SemaphoreType.DMA((cuts, len(jobs)))],
        compiler_params=pltpu.CompilerParams(vmem_limit_bytes=VMEM_BYTES),
        cost_estimate=pl.CostEstimate(flops=rows_in * width, bytes_accessed=4 * rows_in * width, transcendentals=0),
        name="sums",
    )(*arrays)


def _where_kernel(q_ref, k_ref, q_out, k_out):
    q_out[...] = q_ref[...].astype(F32)
    k_out[...] = k_ref[...].astype(F32)


def as_float(q, k):
    return pl.pallas_call(
        _where_kernel,
        in_specs=[pl.BlockSpec(memory_space=pltpu.VMEM)] * 2,
        out_specs=[pl.BlockSpec(memory_space=pltpu.VMEM)] * 2,
        out_shape=[jax.ShapeDtypeStruct(q.shape, F32), jax.ShapeDtypeStruct(k.shape, F32)],
        cost_estimate=pl.CostEstimate(flops=q.size, bytes_accessed=16 * q.size, transcendentals=0),
        name="where",
    )(q, k)


CUTS = (16, 32, 16)
UNITS = U1A, U1B, U2A, U2B, U3A, U3B, U0A, U0B = ("u1a", "u1b", "u2a", "u2b", "u3a", "u3b", "u0a", "u0b")


def solution(mesh):
    n_dev = mesh.shape[AXIS]

    def send(value, mask):
        return lax.ppermute(value, AXIS, [(i, i ^ mask) for i in range(n_dev)])

    def by_mask(arr, me):
        cube = arr.reshape((2, 2, 2) + arr.shape[1:])
        for axis, bit in ((0, 4), (1, 2), (2, 1)):
            cube = jnp.where((me & bit) != 0, jnp.flip(cube, axis), cube)
        return cube.reshape(arr.shape)

    def local_step(x_loc, ln_gain, wq_loc, w_kv, wo_loc, positions):
        me = lax.axis_index(AXIS)
        rows, width = x_loc.shape
        seq = positions.shape[0]
        piece = rows // 4
        gain = ln_gain.reshape(1, width)

        def send_all(values, mask):
            return [send(v, mask) for v in values]

        h, fx, fy, fd = [[] for _ in range(4)], [None] * 4, [None] * 4, [None] * 4
        a, b, _ = CUTS
        early = fetch_first(x_loc, a)
        middle, = norm_rows(x_loc, gain, a, b, 1, a)
        head_rows, tail_rows = norm_rows(x_loc, gain, 0, a, 2, a, (a + b) // a)
        h[0] = [head_rows, middle, tail_rows]
        for i, v in enumerate(norm_rows(x_loc, gain, piece, piece, 3, piece // 2)):
            h[i + 1].append(v)
        k_own, v_own = unit_call(sum(h, []), w_kv, None, None, None, None, None, 0, [rows - piece, rows + piece], slots=4, chunk=2048)
        sent = [[early] + h[0][1:]] + h[1:]
        for i in range(4):
            fx[i], fy[i] = send_all(sent[i], XN), send_all(sent[i], YN)
        for i in (0, 1):
            fd[i] = send_all(fx[i], YN)
        for i in (2, 3):
            fd[i] = send_all(fy[i], XN)
        for far in (fx, fy, fd):
            far[0] = [*norm_rows(far[0][0], gain, 0, a, 1, a), *far[0][1:]]
        k_m, v_m = {0: k_own}, {0: v_own}
        for m in (XN, YN):
            k_m[m], v_m[m] = send(k_own, m), send(v_own, m)
        k_m[DIAG], v_m[DIAG] = send(k_m[XN], YN), send(v_m[YN], XN)
        for m in (0, XN, YN, DIAG):
            k_m[m | CORE], v_m[m | CORE] = send(k_m[m], CORE), send(v_m[m], CORE)
        keys, values = [k_m[m] for m in range(n_dev)], [v_m[m] for m in range(n_dev)]
        k_cache, v_cache = order_blocks(keys, values)

        pos_m = by_mask(positions.reshape(n_dev, 4, piece), me)
        kpos = pos_m.reshape(1, seq)
        plan = {
            U0A: [(0, 0, h[0]), (0, 1, h[1])], U0B: [(0, 2, h[2]), (0, 3, h[3])],
            U1A: [(XN, 0, fx[0]), (YN, 0, fy[0])], U1B: [(XN, 1, fx[1]), (YN, 2, fy[2])],
            U2A: [(XN, 2, fx[2]), (YN, 3, fy[3])], U2B: [(XN, 3, fx[3]), (YN, 1, fy[1])],
            U3A: [(DIAG, 0, fd[0]), (DIAG, 2, fd[2])], U3B: [(DIAG, 1, fd[1]), (DIAG, 3, fd[3])],
        }
        qpos = jnp.concatenate([pos_m[m | c, i] for u in UNITS for c in (0, CORE) for m, i, _ in plan[u]]).reshape(len(UNITS), -1)
        qpos, kpos = as_float(qpos, kpos)

        parts = {}
        for index, name in enumerate(UNITS):
            blocks = plan[name]
            mine = sum((b for _, _, b in blocks), [])
            lhs = mine + send_all(mine, CORE)
            splits = [piece] * len(blocks) + [piece * len(blocks)]
            *own, other = unit_call(lhs, wq_loc, wo_loc, keys, values, qpos, kpos, index, splits)
            back = send(other, CORE)
            for j, (m, i, _) in enumerate(blocks):
                parts[m, i] = [(own[j], 0), (back, j * piece)]

        def total(*jobs):
            return sums([(k, 0, piece, t) for k, t in enumerate(jobs)], [piece] * len(jobs))

        def both(i, j):
            px, py = total(parts[DIAG, i], parts[DIAG, j])
            return send(px, XN), send(py, YN)

        got = {}
        px, = total(parts[XN, 0])
        got[0] = send(px, XN)
        px, py = total(parts[XN, 1], parts[YN, 2])
        got[1], got[2] = send(px, XN), send(py, YN)
        py, = total(parts[YN, 3])
        got[3] = send(py, YN)
        last = []
        for i, j, cuts in ((0, 2, (piece,)), (1, 3, (piece // 2, piece // 4, piece // 8, piece // 8))):
            hx, hy = both(i, j)
            first = 0
            for n in cuts:
                jobs = []
                for k, (p, owner, far) in enumerate(((i, YN, hx), (j, XN, hy))):
                    jobs.append((k, 0, n, [(a, f + first) for a, f in parts[owner, p] + [(far, 0)]]))
                py, px = sums(jobs, [n, n])
                last.append((n, (i * piece + first, send(py, YN)), (j * piece + first, send(px, XN))))
                first += n
        y, = sums([(0, i * piece, piece, parts[0, i] + [(got[i], 0)]) for i in range(4)], [rows])
        for n, *arrived in last:
            y, = sums([(0, f, n, [(y, f), (a, 0)]) for f, a in arrived], [rows], into=y)
        return y, k_cache, v_cache

    return jax.shard_map(
        local_step,
        mesh=mesh,
        in_specs=(P(AXIS, None), P(None), P(None, AXIS), P(None, None), P(AXIS, None), P(None)),
        out_specs=(P(AXIS, None), P(None, None), P(None, None)),
        check_vma=False,
    )
```

```python
import functools
import math

import jax
import jax.numpy as jnp
from jax import lax
from jax.experimental import pallas as pl
from jax.experimental.pallas import tpu as pltpu
from jax.sharding import PartitionSpec as P


NORM_EPS = 1e-6
LOG2E = math.log2(math.e)
VMEM_BYTES = 67043328
NORM_BYTES = 56 << 20
AXIS = "model"
CORE, XN, YN, DIAG = 1, 2, 4, 6
BF16, F32 = jnp.bfloat16, jnp.float32


def _norm_kernel(chunk, steps, x_ref, g_ref, *out_refs):
    rows, width = x_ref.shape
    n_chunks = width // chunk

    def cols(c):
        return pl.ds(pl.multiple_of(c * chunk, chunk), chunk)

    def load(c):
        return x_ref[:, cols(c)].astype(F32)

    def fold(v):
        acc = v[:, :128]
        for i in range(1, chunk // 128):
            acc = acc + v[:, i * 128:(i + 1) * 128]
        return acc

    def square(c, acc):
        d = load(c) - mean
        return acc + fold(d * d)

    zero = jnp.zeros((rows, 128), F32)
    mean = jnp.sum(lax.fori_loop(0, n_chunks, lambda c, acc: acc + fold(load(c)), zero), axis=1, keepdims=True) / width
    rstd = lax.rsqrt(jnp.sum(lax.fori_loop(0, n_chunks, square, zero), axis=1, keepdims=True) / width + NORM_EPS)
    for i, out_ref in enumerate(out_refs):
        @pl.when(pl.program_id(0) // steps == i)
        def _():
            def put(c, _):
                out_ref[:, cols(c)] = ((load(c) - mean) * rstd * g_ref[:, cols(c)]).astype(BF16)
                return 0

            lax.fori_loop(0, n_chunks, put, 0)


def _fetch_kernel(x_hbm, out_ref, sem):
    copy = pltpu.make_async_copy(x_hbm.at[pl.ds(0, out_ref.shape[0]), :], out_ref, sem)
    copy.start()
    copy.wait()


def fetch_first(x, rows):
    return pl.pallas_call(
        _fetch_kernel,
        in_specs=[pl.BlockSpec(memory_space=pltpu.HBM)],
        out_specs=pl.BlockSpec(memory_space=pltpu.VMEM),
        out_shape=pltpu.VMEM((rows, x.shape[1]), BF16),
        scratch_shapes=[pltpu.SemaphoreType.DMA],
        compiler_params=pltpu.CompilerParams(vmem_limit_bytes=NORM_BYTES),
        cost_estimate=pl.CostEstimate(flops=rows * x.shape[1], bytes_accessed=4 * rows * x.shape[1], transcendentals=0),
        name="fetch",
    )(x)


def norm_rows(x, gain, first, piece, count, rows, stride=1):
    width = x.shape[1]
    steps = piece // rows

    def out_map(i):
        return lambda s: (jnp.clip(s - i * steps, 0, steps - 1), 0)

    return pl.pallas_call(
        functools.partial(_norm_kernel, 2048, steps),
        grid=(count * steps,),
        in_specs=[pl.BlockSpec((rows, width), lambda s: (first // rows + stride * s, 0)), pl.BlockSpec((1, width), lambda s: (0, 0))],
        out_specs=[pl.BlockSpec((rows, width), out_map(i)) for i in range(count)],
        out_shape=[jax.ShapeDtypeStruct((piece, width), BF16)] * count,
        compiler_params=pltpu.CompilerParams(dimension_semantics=("arbitrary",), vmem_limit_bytes=NORM_BYTES),
        cost_estimate=pl.CostEstimate(flops=8 * count * piece * width, bytes_accessed=4 * count * piece * width, transcendentals=0),
        name="norm",
    )(x, gain)


def _order_kernel(moves, per, *refs):
    me = lax.axis_index(AXIS)
    for src, first, n, which, m, row in moves:
        to = pl.multiple_of((me ^ m) * per + row, 16)
        refs[which - 2][pl.ds(to, n), :] = refs[src][first:first + n, :]


def order_blocks(sources, moves, per, total):
    cols = sources[0].shape[1]
    return pl.pallas_call(
        functools.partial(_order_kernel, moves, per),
        in_specs=[pl.BlockSpec(memory_space=pltpu.VMEM)] * len(sources),
        out_specs=[pl.BlockSpec(memory_space=pltpu.VMEM)] * 2,
        out_shape=[jax.ShapeDtypeStruct((total, cols), BF16)] * 2,
        cost_estimate=pl.CostEstimate(flops=2 * total * cols, bytes_accessed=8 * total * cols, transcendentals=0),
        name="order",
    )(*sources)


def _unit_kernel(names, parts, n_lhs, n_out, index, moves, picks, *flat):
    r = dict(zip(names, flat))
    lhs = [r[f"lhs{i}"] for i in range(n_lhs)]
    outs = [r[f"out{i}"] for i in range(n_out)]
    ring, ring_sem, q_buf = r["ring"], r["ring_sem"], r["q_buf"]
    slots, chunk = ring.shape[:2]
    do_q, do_o = "q" in parts, "o" in parts
    rows, proj = q_buf.shape
    n_q = r["wq"].shape[0] // chunk if do_q else 0
    n_o = r["wo"].shape[1] // chunk if do_o else 0
    total = n_q + n_o

    def at(i):
        return pl.ds(pl.multiple_of(i * chunk, chunk), chunk)

    def wq_copy(i, slot):
        return pltpu.make_async_copy(r["wq"].at[at(i), :], ring.at[slot], ring_sem.at[slot])

    def wo_copy(i, slot):
        return pltpu.make_async_copy(r["wo"].at[:, at(i - n_q)], ring.at[slot], ring_sem.at[slot])

    def h_copies(i, slot):
        cps, first = [], 0
        for j, h in enumerate(lhs):
            n = h.shape[0]
            cps.append(pltpu.make_async_copy(h.at[:, at(i)], r["h_buf"].at[slot, pl.ds(first, n), :], r["h_sem"].at[slot, j]))
            first += n
        return cps

    def y_copies(i, slot):
        cps, first = [], 0
        for j, out in enumerate(outs):
            n = out.shape[0]
            cps.append(pltpu.make_async_copy(r["y_buf"].at[slot, pl.ds(first, n), :], out.at[:, at(i)], r["y_sem"].at[slot, j]))
            first += n
        return cps

    def fetch(i, slot):
        if do_q:
            @pl.when(i < n_q)
            def _():
                wq_copy(i, slot).start()
                for c in h_copies(i, slot):
                    c.start()
        if do_o:
            @pl.when((i >= n_q) & (i < total))
            def _():
                wo_copy(i, slot).start()

    for i in range(slots):
        if i < n_q:
            wq_copy(i, i).start()
            for c in h_copies(i, i):
                c.start()
        elif i < total:
            wo_copy(i, i).start()
    extra = []
    if do_o:
        block = r["qpos"].shape[1]
        row, col = (lax.broadcasted_iota(jnp.int32, (block, block), d) for d in (0, 1))
        for i in range(rows // block):
            mine = jnp.where(row == col, r["qpos"][index + i:index + i + 1, :], 0.0)
            r["q_col"][pl.ds(i * block, block), :] = jnp.sum(mine, axis=1, keepdims=True)
        for i, (src, first, n, which, at_row) in enumerate(moves):
            buf = r["v_buf"] if which else r["k_buf"]
            extra.append(pltpu.make_async_copy(r[f"s{src}"].at[pl.ds(first, n), :], buf.at[pl.ds(at_row, n), :], r["kv_sem"].at[i]))
        if not do_q:
            extra.append(pltpu.make_async_copy(lhs[0], q_buf, r["kv_sem"].at[len(moves)]))
    for c in extra:
        c.start()

    if do_q:
        acc = r["acc"]
        acc[...] = jnp.zeros_like(acc)

        def q_step(i, _):
            slot = lax.rem(i, slots)
            wq_copy(i, slot).wait()
            for c in h_copies(i, slot):
                c.wait()
            acc[...] += jnp.dot(r["h_buf"][slot], ring[slot], preferred_element_type=F32)
            fetch(i + slots, slot)
            return 0

        lax.fori_loop(0, n_q, q_step, 0)
        if not do_o:
            for out, to, first, n, left in picks:
                cols = outs[out].shape[1]
                outs[out][pl.ds(to, n), :] = acc[pl.ds(first, n), left:left + cols].astype(BF16)
            return
        q_buf[...] = acc[...].astype(BF16)

    for c in extra:
        c.wait()
    k_buf, v_buf, o_buf, y_buf = r["k_buf"], r["v_buf"], r["o_buf"], r["y_buf"]
    head = k_buf.shape[1]
    heads = proj // head

    half = rows // 2

    def score(s_ref, n, b):
        cols = pl.ds(pl.multiple_of(n * head, head), head)
        s_ref[...] = lax.dot_general(q_buf[pl.ds(b * half, half), cols], k_buf[...], (((1,), (1,)), ((), ())), preferred_element_type=F32)

    def attend(s_ref, n, b):
        mine, cols = pl.ds(b * half, half), pl.ds(pl.multiple_of(n * head, head), head)
        s = jnp.where(r["kpos"][...] <= r["q_col"][mine, :], s_ref[...], -1e30)
        e = jnp.exp2((s - jnp.max(s, axis=-1, keepdims=True)) * (head ** -0.5 * LOG2E))
        p = (e * (1.0 / jnp.sum(e, axis=-1, keepdims=True))).astype(BF16)
        o_buf[mine, cols] = jnp.dot(p, v_buf[...], preferred_element_type=F32).astype(BF16)

    def one_head(n, _):
        score(r["s_b"], n, 1)
        attend(r["s_a"], n, 0)
        score(r["s_a"], jnp.minimum(n + 1, heads - 1), 0)
        attend(r["s_b"], n, 1)
        return 0

    score(r["s_a"], 0, 0)
    lax.fori_loop(0, heads, one_head, 0)

    def o_step(i, _):
        slot, yslot = lax.rem(n_q + i, slots), lax.rem(i, 2)
        wo_copy(n_q + i, slot).wait()

        @pl.when(i >= 2)
        def _():
            for c in y_copies(i - 2, yslot):
                c.wait()

        y_buf[yslot] = jnp.dot(o_buf[...], ring[slot], preferred_element_type=F32).astype(BF16)
        for c in y_copies(i, yslot):
            c.start()
        fetch(n_q + i + slots, slot)
        return 0

    lax.fori_loop(0, n_o, o_step, 0)
    for i in (n_o - 2, n_o - 1):
        for c in y_copies(i, i % 2):
            c.wait()


def unit_call(lhs, wq, wo, keys, qpos, kpos, index, splits, picks=(), slots=7, chunk=None):
    parts = ("q" if wq is not None else "") + ("o" if wo is not None else "")
    rows = sum(h.shape[0] for h in lhs)
    proj, width = (wq.shape[1], wq.shape[0]) if wq is not None else wo.shape
    chunk = chunk or proj
    any_ = pl.BlockSpec(memory_space=pl.ANY)
    ins = [(f"lhs{i}", h, any_) for i, h in enumerate(lhs)]
    moves = ()
    scratch = [("ring", pltpu.VMEM((slots, chunk, proj), BF16)), ("ring_sem", pltpu.SemaphoreType.DMA((slots,))), ("q_buf", pltpu.VMEM((rows, proj), BF16))]
    flops, moved = 0, 0
    if wq is not None:
        ins.append(("wq", wq, any_))
        scratch += [("h_buf", pltpu.VMEM((slots, rows, chunk), BF16)), ("h_sem", pltpu.SemaphoreType.DMA((slots, len(lhs)))), ("acc", pltpu.VMEM((rows, proj), F32))]
        flops += 2 * rows * proj * width
        moved += 2 * (rows + proj) * width
    if wo is not None:
        sources, at = keys
        n_keys, head = kpos.shape[1], sources[0].shape[1]
        per = n_keys // (1 + max(m for _, _, _, _, m, _ in at))
        moves = tuple((src, first, n, which, m * per + row) for src, first, n, which, m, row in at)
        ins.append(("wo", wo, any_))
        ins += [(f"s{i}", a, any_) for i, a in enumerate(sources)]
        ins += [("qpos", qpos, pl.BlockSpec(qpos.shape, lambda i: (0, 0))), ("kpos", kpos, pl.BlockSpec((1, n_keys), lambda i: (0, 0)))]
        scratch += [
            ("o_buf", pltpu.VMEM((rows, proj), BF16)), ("y_buf", pltpu.VMEM((2, rows, chunk), BF16)), ("y_sem", pltpu.SemaphoreType.DMA((2, len(splits)))),
            ("q_col", pltpu.VMEM((rows, 1), F32)), ("s_a", pltpu.VMEM((rows // 2, n_keys), F32)), ("s_b", pltpu.VMEM((rows // 2, n_keys), F32)),
            ("k_buf", pltpu.VMEM((n_keys, head), BF16)), ("v_buf", pltpu.VMEM((n_keys, head), BF16)), ("kv_sem", pltpu.SemaphoreType.DMA((len(moves) + 1,))),
        ]
        flops += 2 * rows * proj * (width + 2 * n_keys)
        moved += 2 * (rows + proj) * width
        outs = [((n, width), any_) for n in splits]
    else:
        outs = [(n, pl.BlockSpec(n, lambda i: (0, 0))) for n in splits]
    names = [i[0] for i in ins] + [f"out{i}" for i in range(len(outs))] + [s[0] for s in scratch]
    res = pl.pallas_call(
        functools.partial(_unit_kernel, names, parts, len(lhs), len(outs), index, moves, tuple(picks)),
        grid=(1,),
        in_specs=[i[2] for i in ins],
        out_specs=[o[1] for o in outs],
        out_shape=[jax.ShapeDtypeStruct(o[0], BF16) for o in outs],
        scratch_shapes=[s[1] for s in scratch],
        compiler_params=pltpu.CompilerParams(dimension_semantics=("arbitrary",), vmem_limit_bytes=VMEM_BYTES if wo is not None else NORM_BYTES),
        cost_estimate=pl.CostEstimate(flops=flops, bytes_accessed=moved, transcendentals=0),
    )(*[i[1] for i in ins])
    return res


def _sums_kernel(jobs, n_in, *refs):
    ins, outs, bufs, in_sem, out_sem = refs[:n_in], refs[n_in:-3], refs[-3], refs[-2], refs[-1]
    halves = in_sem.shape[0]
    width = bufs.shape[1] // halves
    loads, stores, slots = {}, [], []
    at = 0
    for out, first, rows, terms in jobs:
        slots.append([])
        for _ in terms:
            slots[-1].append(at)
            at += rows
    n = 0
    for c in range(halves):
        cols = pl.ds(c * width, width)
        n = 0
        for j, (_, _, rows, terms) in enumerate(jobs):
            for i, (ref, first) in enumerate(terms):
                loads[c, j, i] = pltpu.make_async_copy(ins[ref].at[pl.ds(first, rows), cols], bufs.at[pl.ds(slots[j][i], rows), cols], in_sem.at[c, n])
                loads[c, j, i].start()
                n += 1
    for c in range(halves):
        for j, (out, first, rows, terms) in enumerate(jobs):
            for i in range(len(terms)):
                loads[c, j, i].wait()

            def some(k, _):
                cols = pl.ds(pl.multiple_of(c * width + k * 512, 512), 512)
                total = bufs[pl.ds(slots[j][0], rows), cols].astype(F32)
                for at in slots[j][1:]:
                    total = total + bufs[pl.ds(at, rows), cols].astype(F32)
                bufs[pl.ds(slots[j][0], rows), cols] = total.astype(BF16)
                return 0

            lax.fori_loop(0, width // 512, some, 0)
            cols = pl.ds(c * width, width)
            stores.append(pltpu.make_async_copy(bufs.at[pl.ds(slots[j][0], rows), cols], outs[out].at[pl.ds(first, rows), cols], out_sem.at[c, j]))
            stores[-1].start()
    for c in stores:
        c.wait()


def sums(jobs, out_rows, into=None):
    arrays = [] if into is None else [into]
    spec = []
    for out, first, rows, terms in jobs:
        at = []
        for a, f in terms:
            k = next((k for k, b in enumerate(arrays) if b is a), len(arrays))
            if k == len(arrays):
                arrays.append(a)
            at.append((k, f))
        spec.append((out, first, rows, tuple(at)))
    width = arrays[0].shape[1]
    n_terms = sum(len(j[3]) for j in jobs)
    rows_in = sum(j[2] * len(j[3]) for j in jobs)
    cuts = 1 if rows_in <= 32 else 2
    any_ = pl.BlockSpec(memory_space=pl.ANY)
    return pl.pallas_call(
        functools.partial(_sums_kernel, tuple(spec), len(arrays)),
        in_specs=[any_] * len(arrays),
        out_specs=[any_] * len(out_rows),
        out_shape=[jax.ShapeDtypeStruct((r, width), BF16) for r in out_rows],
        input_output_aliases={} if into is None else {0: 0},
        scratch_shapes=[pltpu.VMEM((rows_in, width), BF16), pltpu.SemaphoreType.DMA((cuts, n_terms)), pltpu.SemaphoreType.DMA((cuts, len(jobs)))],
        compiler_params=pltpu.CompilerParams(vmem_limit_bytes=VMEM_BYTES),
        cost_estimate=pl.CostEstimate(flops=rows_in * width, bytes_accessed=4 * rows_in * width, transcendentals=0),
        name="sums",
    )(*arrays)


def _where_kernel(q_ref, k_ref, q_out, k_out):
    q_out[...] = q_ref[...].astype(F32)
    k_out[...] = k_ref[...].astype(F32)


def as_float(q, k):
    return pl.pallas_call(
        _where_kernel,
        in_specs=[pl.BlockSpec(memory_space=pltpu.VMEM)] * 2,
        out_specs=[pl.BlockSpec(memory_space=pltpu.VMEM)] * 2,
        out_shape=[jax.ShapeDtypeStruct(q.shape, F32), jax.ShapeDtypeStruct(k.shape, F32)],
        cost_estimate=pl.CostEstimate(flops=q.size, bytes_accessed=16 * q.size, transcendentals=0),
        name="where",
    )(q, k)


CUTS = (16, 32, 16)
UNITS = U1A, U1B, U2A, U3A, U3B, U2B, U0 = ("u1a", "u1b", "u2a", "u3a", "u3b", "u2b", "u0")


def solution(mesh):
    n_dev = mesh.shape[AXIS]

    def send(value, mask):
        return lax.ppermute(value, AXIS, [(i, i ^ mask) for i in range(n_dev)])

    def by_mask(arr, me):
        cube = arr.reshape((2, 2, 2) + arr.shape[1:])
        for axis, bit in ((0, 4), (1, 2), (2, 1)):
            cube = jnp.where((me & bit) != 0, jnp.flip(cube, axis), cube)
        return cube.reshape(arr.shape)

    def local_step(x_loc, ln_gain, wq_loc, w_kv, wo_loc, positions):
        me = lax.axis_index(AXIS)
        rows, width = x_loc.shape
        seq, head = positions.shape[0], w_kv.shape[1] // 2
        piece = rows // 4
        gain = ln_gain.reshape(1, width)

        def send_all(values, mask):
            return [send(v, mask) for v in values]

        h, fx, fy, fd = [[] for _ in range(4)], [None] * 4, [None] * 4, [None] * 4
        a, b, c = CUTS
        early = fetch_first(x_loc, a)
        middle, = norm_rows(x_loc, gain, a, b, 1, a)
        head_rows, tail_rows = norm_rows(x_loc, gain, 0, a, 2, a, (a + b) // a)
        h[0] = [head_rows, middle, tail_rows]
        for i, v in enumerate(norm_rows(x_loc, gain, piece, piece, 3, piece // 2)):
            h[i + 1].append(v)
        low, t = rows - piece, piece
        own_top, own_rest, own_first = unit_call(
            sum(h, []), w_kv, None, None, None, None, 0, [(low - t, head), (low + t, head), (2 * piece, head)],
            picks=((0, 0, piece, low - t, 0), (1, 0, piece, low, head), (1, low, rows - t, t, 0), (2, 0, 0, piece, 0), (2, piece, 0, piece, head)),
            slots=4, chunk=2048,
        )
        sent = [[early] + h[0][1:]] + h[1:]
        for i in range(4):
            fx[i], fy[i] = send_all(sent[i], XN), send_all(sent[i], YN)
        for i in (0, 1):
            fd[i] = send_all(fx[i], YN)
        for i in (2, 3):
            fd[i] = send_all(fy[i], XN)
        for far in (fx, fy, fd):
            far[0] = [*norm_rows(far[0][0], gain, 0, a, 1, a), *far[0][1:]]
        swaps = {}

        def swap(values, name):
            if name not in swaps:
                swaps[name] = send_all(values, CORE)
            return swaps[name]

        mine = fx[0] + fy[0]
        near, near_k, near_v = unit_call(
            mine + swap(mine, U1A), w_kv, None, None, None, None, 0, [(8 * piece, head), (piece, head), (piece, head)],
            picks=((0, 0, 0, 4 * piece, 0), (0, 4 * piece, 0, 4 * piece, head), (1, 0, 0, piece, 0), (2, 0, piece, piece, head)),
            slots=4, chunk=2048,
        )
        top, rest = {0: own_top}, {0: own_rest}
        for m in (XN, YN):
            top[m], rest[m] = send(own_top, m), send(own_rest, m)
        top[DIAG], rest[DIAG] = send(top[XN], YN), send(rest[YN], XN)
        far_k, far_v = send(near_k, YN), send(near_v, XN)
        sources, moves = [near], []

        def found(array, *ranges):
            moves.extend((len(sources),) + x for x in ranges)
            sources.append(array)

        for m in (0, XN, YN, DIAG):
            for c in (0, CORE):
                far = m | c
                upper, lower = (send(v, CORE) for v in (top[m], rest[m])) if c else (top[m], rest[m])
                found(upper, (0, low - t, 0, far, piece))
                found(lower, (0, low, 1, far, piece), (low, t, 0, far, rows - t))
                if m == 0:
                    found(send(own_first, CORE) if c else own_first, (0, piece, 0, far, 0), (piece, piece, 1, far, 0))
                elif m == DIAG:
                    found(send(far_k, CORE) if c else far_k, (0, piece, 0, far, 0))
                    found(send(far_v, CORE) if c else far_v, (0, piece, 1, far, 0))
                else:
                    first = ((m == YN) + 2 * c) * piece
                    moves.extend(((0, first, piece, 0, far, 0), (0, 4 * piece + first, piece, 1, far, 0)))
        k_cache, v_cache = order_blocks(sources, tuple(moves), rows, seq)

        pos_m = by_mask(positions.reshape(n_dev, 4, piece), me)
        kpos = pos_m.reshape(1, seq)
        plan = {
            U0: [(0, i, h[i]) for i in range(4)],
            U1A: [(XN, 0, fx[0]), (YN, 0, fy[0])], U1B: [(XN, 1, fx[1]), (YN, 2, fy[2])],
            U2A: [(XN, 2, fx[2]), (YN, 3, fy[3])], U2B: [(XN, 3, fx[3]), (YN, 1, fy[1])],
            U3A: [(DIAG, 0, fd[0]), (DIAG, 2, fd[2])], U3B: [(DIAG, 1, fd[1]), (DIAG, 3, fd[3])],
        }
        qpos = jnp.concatenate([pos_m[m | c, i] for u in UNITS for c in (0, CORE) for m, i, _ in plan[u]]).reshape(-1, rows)
        qpos, kpos = as_float(qpos, kpos)

        parts = {}
        for index, name in enumerate(UNITS):
            blocks = plan[name]
            mine = sum((b for _, _, b in blocks), [])
            lhs, wq = mine + swap(mine, name), wq_loc
            if name == U0:
                total_rows, width_q = 2 * rows, wq_loc.shape[1]
                lhs = unit_call(lhs, wq_loc, None, None, None, None, 0, [(total_rows, width_q)], picks=((0, 0, 0, total_rows, 0),), slots=4)
                wq = None
            splits = [piece] * len(blocks) + [piece * len(blocks)]
            *own, other = unit_call(lhs, wq, wo_loc, (sources, moves), qpos, kpos, index, splits)
            back = send(other, CORE)
            for j, (m, i, _) in enumerate(blocks):
                parts[m, i] = [(own[j], 0), (back, j * piece)]

        def total(*jobs):
            return sums([(k, 0, piece, t) for k, t in enumerate(jobs)], [piece] * len(jobs))

        def both(i, j):
            px, py = total(parts[DIAG, i], parts[DIAG, j])
            return send(px, XN), send(py, YN)

        got = {}
        px, = total(parts[XN, 0])
        got[0] = send(px, XN)
        px, py = total(parts[XN, 1], parts[YN, 2])
        got[1], got[2] = send(px, XN), send(py, YN)
        py, = total(parts[YN, 3])
        got[3] = send(py, YN)
        last = []
        for i, j, cuts in ((0, 2, (piece,)), (1, 3, (piece // 2, piece // 4, piece // 8, piece // 8))):
            hx, hy = both(i, j)
            first = 0
            for n in cuts:
                jobs = []
                for k, (p, owner, far) in enumerate(((i, YN, hx), (j, XN, hy))):
                    jobs.append((k, 0, n, [(a, f + first) for a, f in parts[owner, p] + [(far, 0)]]))
                py, px = sums(jobs, [n, n])
                last.append((n, (i * piece + first, send(py, YN)), (j * piece + first, send(px, XN))))
                first += n
        y, = sums([(0, i * piece, piece, parts[0, i] + [(got[i], 0)]) for i in range(4)], [rows])
        for n, *arrived in last:
            y, = sums([(0, f, n, [(y, f), (a, 0)]) for f, a in arrived], [rows], into=y)
        return y, k_cache, v_cache

    return jax.shard_map(
        local_step,
        mesh=mesh,
        in_specs=(P(AXIS, None), P(None), P(None, AXIS), P(None, None), P(AXIS, None), P(None)),
        out_specs=(P(AXIS, None), P(None, None), P(None, None)),
        check_vma=False,
    )
```
